32 devices in a mesh: seq: 8 (over z, x), feat: 4 (over y, core).
Axes of the slice: x: 2, y: 2, z: 4, core: 2. Of those that a mesh axis runs over, the one named last changes fastest.
Arguments:
- injection: bfloat16 [1024, 5120], P('seq', 'feat'), may hold values from -8 to 8
- warm_start: bfloat16 [1024, 5120], P('seq', 'feat'), may hold values from -12 to 12
- gain_in: float32 [5120], replicated, may hold values from 0.5 to 1.5
- gain_out: float32 [5120], replicated, may hold values from 0.5 to 1.5
- w_query: bfloat16 [5120, 5120], P(None, 'feat'), may hold values from -0.0848993624 to 0.0848993624
- w_key: bfloat16 [5120, 1024], P(None, 'feat'), may hold values from -0.0848993624 to 0.0848993624
- w_value: bfloat16 [5120, 1024], P(None, 'feat'), may hold values from -0.078125 to 0.078125
- w_out: bfloat16 [5120, 5120], P('feat'), may hold values from -0.078125 to 0.078125
Outputs:
- equilibrium: float32 [1024, 5120], P('seq', 'feat')
The draws below stay inside these ranges and needn't reach their ends.
All inputs are finite; a program needn't handle non-finite values.
Results may differ from the reference program's by a relative error of at most 0.009.
Values may be sent and summed in bfloat16 or wider, within the bound.
A program may use at most 128 MiB of HBM per device.

```python
import math
import jax
import jax.numpy as jnp
from jax import lax

D = 5120
HEADS = 40
KV_HEADS = 8
HEAD_DIM = 128
ITERS = 4
TOKENS = 1024


ALIGN_TARGET = 325.0


def align_scale():
    return math.sqrt(ALIGN_TARGET / (D * math.sqrt(HEAD_DIM)))


def spike_layout(key):
    sign_query = jax.random.randint(jax.random.fold_in(key, 7001), (D,), 0, 2).astype(jnp.float32) * 2.0 - 1.0
    sign_key = jax.random.randint(jax.random.fold_in(key, 7002), (D,), 0, 2).astype(jnp.float32) * 2.0 - 1.0
    half_tokens = TOKENS // 2
    key_places = jax.random.permutation(jax.random.fold_in(key, 7003), half_tokens)[:8].astype(jnp.int32)
    query_places = (jax.random.permutation(jax.random.fold_in(key, 7004), half_tokens)[:8] + half_tokens).astype(jnp.int32)
    return (sign_query, sign_key, key_places, query_places)


def matrix_noise(key, columns):
    noise_part = jnp.clip(jax.random.normal(key, (D, columns), jnp.float32), -6.0, 6.0)
    return noise_part / math.sqrt(D)


def draw_injection(key, part):
    sign_query, sign_key, key_places, query_places = spike_layout(key)
    base_noise = jnp.clip(jax.random.normal(jax.random.fold_in(key, 11), (TOKENS, D), jnp.float32), -4.0, 4.0)
    position = jnp.arange(TOKENS, dtype=jnp.int32)
    query_strength = jnp.array([0.5, 0.5, 1.0, 1.0, 2.0, 2.0, 4.0, 4.0], jnp.float32)
    query_weight = jnp.sum(jnp.where(position[None, :] == query_places[:, None], query_strength[:, None], 0.0), axis=0)
    key_weight = jnp.sum(jnp.where(position[None, :] == key_places[:, None], 3.0, 0.0), axis=0)
    result = base_noise + query_weight[:, None] * sign_query[None, :] + key_weight[:, None] * sign_key[None, :]
    return result.astype(jnp.bfloat16)


def draw_w_query(key, part):
    sign_query, sign_key, key_places, query_places = spike_layout(key)
    noise_part = matrix_noise(jax.random.fold_in(key, 21), HEADS * HEAD_DIM)
    result = noise_part + align_scale() * sign_query[:, None] / math.sqrt(D)
    return result.astype(jnp.bfloat16)


def draw_w_key(key, part):
    sign_query, sign_key, key_places, query_places = spike_layout(key)
    noise_part = matrix_noise(jax.random.fold_in(key, 22), KV_HEADS * HEAD_DIM)
    result = noise_part + align_scale() * sign_key[:, None] / math.sqrt(D)
    return result.astype(jnp.bfloat16)


def draw_warm_start(key, part):
    row_frac = jnp.arange(TOKENS, dtype=jnp.float32) / (TOKENS - 1)
    col_frac = jnp.arange(D, dtype=jnp.float32) / (D - 1)
    row_rough = jnp.exp(jax.random.uniform(jax.random.fold_in(key, 31), (TOKENS,), jnp.float32, math.log(0.7), math.log(1.4)))
    col_rough = jnp.exp(jax.random.uniform(jax.random.fold_in(key, 32), (D,), jnp.float32, math.log(0.7), math.log(1.4)))
    col_scale = (0.6 + 0.9 * col_frac) * col_rough
    base_noise = jnp.clip(jax.random.normal(jax.random.fold_in(key, 33), (TOKENS, D), jnp.float32), -4.0, 4.0)
    row_scale = jnp.exp(math.log(0.25) + row_frac * math.log(10.0)) * row_rough
    result = base_noise * row_scale[:, None] * col_scale[None, :]
    return jnp.clip(result, -12.0, 12.0).astype(jnp.bfloat16)


def shard_levels(stream_key, shape, cuts, smallest, largest):
    loudness, own = 1.0, jax.random.fold_in(stream_key, 6)
    for dim, parts in cuts:
        heights = jnp.exp(jax.random.uniform(jax.random.fold_in(own, dim), (parts,), jnp.float32, smallest / len(cuts), largest / len(cuts)))
        loudness = loudness * jnp.repeat(heights, shape[dim] // parts).reshape([-1 if axis == dim else 1 for axis in range(len(shape))])
    return loudness


def centred(own_key, dims, width, limit, pieces=(), kind=jnp.bfloat16):
    values = jax.random.normal(own_key, dims, jnp.float32) * width
    if len(pieces) > 0:
        values = shard_levels(own_key, dims, pieces, -0.22, 0.18) * values
    return jnp.clip(values, min=-limit, max=limit).astype(kind)


def setup_inputs(seed: int = 0) -> dict:
    splits = jax.random.split(jax.random.key(seed), 9)
    return {
        "injection": draw_injection(jax.random.fold_in(splits[8], 71), 0),
        "warm_start": draw_warm_start(jax.random.fold_in(splits[8], 71), 0),
        "gain_in": jnp.clip(1.0 + 0.1 * jax.random.normal(splits[2], (D,), jnp.float32), 0.5, 1.5),
        "gain_out": jnp.clip(1.0 + 0.1 * jax.random.normal(splits[3], (D,), jnp.float32), 0.5, 1.5),
        "w_query": draw_w_query(jax.random.fold_in(splits[8], 71), 0),
        "w_key": draw_w_key(jax.random.fold_in(splits[8], 71), 0),
        "w_value": centred(splits[6], (D, KV_HEADS * HEAD_DIM), D ** -0.5, 0.078125, ((1, 4),)),
        "w_out": centred(splits[7], (HEADS * HEAD_DIM, D), (HEADS * HEAD_DIM) ** -0.5, 0.078125, ((0, 4),)),
    }


EPS = 1e-06
LAMBDA = 0.03

def rms_scale(matrix, gain_vec):
    return matrix * lax.rsqrt(lax.optimization_barrier(jnp.mean(matrix * matrix, axis=-1, keepdims=True)) + EPS) * gain_vec

def solve_small(matrix, target):
    size_now = target.shape[0]
    row_list = [matrix[idx_row] for idx_row in range(size_now)]
    value_list = [target[idx_row] for idx_row in range(size_now)]
    for pivot_at in range(size_now):
        for below_at in range(pivot_at + 1, size_now):
            ratio_now = row_list[below_at][pivot_at] / row_list[pivot_at][pivot_at]
            row_list[below_at] = row_list[below_at] - ratio_now * row_list[pivot_at]
            value_list[below_at] = value_list[below_at] - ratio_now * value_list[pivot_at]
    result_list = [None] * size_now
    for pivot_at in reversed(range(size_now)):
        running = value_list[pivot_at]
        for later_at in range(pivot_at + 1, size_now):
            running = running - row_list[pivot_at][later_at] * result_list[later_at]
        result_list[pivot_at] = running / row_list[pivot_at][pivot_at]
    return jnp.stack(result_list)

def coefficients(gram_matrix):
    history_len = gram_matrix.shape[0]
    system = gram_matrix / (TOKENS * D) + LAMBDA * jnp.eye(history_len, dtype=jnp.float32)
    unscaled = solve_small(system, jnp.ones((history_len,), jnp.float32))
    return unscaled / jnp.sum(unscaled)

def layer(current, injection, gain_in, gain_out, w_query, w_key, w_value, w_out):
    group = HEADS // KV_HEADS
    mixed = current + injection.astype(jnp.float32)
    normed = rms_scale(mixed, gain_in).astype(jnp.bfloat16)
    queries = jnp.dot(normed, w_query, preferred_element_type=jnp.float32).astype(jnp.bfloat16)
    key_rows = jnp.dot(normed, w_key, preferred_element_type=jnp.float32).astype(jnp.bfloat16)
    value_rows = jnp.dot(normed, w_value, preferred_element_type=jnp.float32).astype(jnp.bfloat16)
    queries = queries.reshape(TOKENS, KV_HEADS, group, HEAD_DIM).transpose(1, 2, 0, 3)
    key_rows = key_rows.reshape(TOKENS, KV_HEADS, HEAD_DIM).transpose(1, 0, 2)
    value_rows = value_rows.reshape(TOKENS, KV_HEADS, HEAD_DIM).transpose(1, 0, 2)
    position = jnp.arange(TOKENS, dtype=jnp.int32)
    allowed = position[:, None] >= position[None, :]
    score_scale = 1.0 / math.sqrt(HEAD_DIM)

    def one_head(operands):
        query_head, key_head, value_head = operands
        scores = jnp.einsum('gtd,sd->gts', query_head.astype(jnp.float32), key_head.astype(jnp.float32)) * score_scale
        scores = jnp.where(allowed[None], scores, -1e+30)
        row_max = lax.optimization_barrier(jnp.max(scores, axis=-1, keepdims=True))
        weights = jnp.where(allowed[None], jnp.exp(scores - row_max), 0.0)
        row_sum = lax.optimization_barrier(jnp.sum(weights, axis=-1, keepdims=True))
        summed = jnp.einsum('gts,sd->gtd', weights.astype(jnp.bfloat16).astype(jnp.float32), value_head.astype(jnp.float32))
        return (summed / row_sum).astype(jnp.bfloat16)
    attended = lax.map(one_head, (queries, key_rows, value_rows))
    attended = attended.transpose(2, 0, 1, 3).reshape(TOKENS, HEADS * HEAD_DIM)
    update = jnp.dot(attended, w_out, preferred_element_type=jnp.float32)
    return rms_scale(mixed + update, gain_out)

def reference(injection, warm_start, gain_in, gain_out, w_query, w_key, w_value, w_out):
    params = (injection, gain_in, gain_out, w_query, w_key, w_value, w_out)
    current = warm_start.astype(jnp.float32)
    evaluated = []
    residuals = []
    for iteration in range(ITERS):
        image = layer(current, *params)
        evaluated.append(image)
        residuals.append(image - current)
        if iteration == 0:
            current = image
        else:
            history_len = iteration + 1
            gram_matrix = jnp.stack([jnp.stack([jnp.sum(residuals[row_at] * residuals[col_at]) for col_at in range(history_len)]) for row_at in range(history_len)])
            weights_now = coefficients(gram_matrix)
            current = weights_now[0] * evaluated[0]
            for other in range(1, history_len):
                current = current + weights_now[other] * evaluated[other]
    return current
```

```python
import functools
import math

import jax
import jax.numpy as jnp
from jax import lax
from jax.experimental import pallas as pl
from jax.experimental.pallas import tpu as pltpu
from jax.sharding import PartitionSpec as P

HEADS = 40
KV_HEADS = 8
HEAD_DIM = 128
ITERS = 4

EPS = 1e-06
LAMBDA = 0.03
CHUNKS = 5
HALVES = 2
MESH = pl.DeviceIdType.MESH
VMEM = pl.BlockSpec(memory_space=pltpu.VMEM)
ANY = pl.BlockSpec(memory_space=pl.ANY)


def remote(src, dst, send_sem, recv_sem, axis, target):
    return pltpu.make_async_remote_copy(
        src_ref=src, dst_ref=dst, send_sem=send_sem, recv_sem=recv_sem,
        device_id={axis: target}, device_id_type=MESH,
    )


def solve_values(rows, values):
    size = len(values)
    rows = [list(row) for row in rows]
    values = list(values)
    for pivot in range(size):
        for below in range(pivot + 1, size):
            ratio = rows[below][pivot] / rows[pivot][pivot]
            for at in range(pivot, size):
                rows[below][at] = rows[below][at] - ratio * rows[pivot][at]
            values[below] = values[below] - ratio * values[pivot]
    result = [None] * size
    for pivot in reversed(range(size)):
        running = values[pivot]
        for later in range(pivot + 1, size):
            running = running - rows[pivot][later] * result[later]
        result[pivot] = running / rows[pivot][pivot]
    return result


def whole_kernel(n, m, inj_hbm, warm_hbm, gain_in, gain_out, wq_hbm, wk_hbm, wv_hbm, wo_hbm, out,
                 tok, tok_inj, w_kv, w_q, w_o, inj, warm, images, residuals, held, proj, queries, kv,
                 acc, top, bias, attended, keep, near_out, near, outgoing, far, coef, gram,
                 scale_out, scale_in, mail_out, mail, wide_out, wide,
                 load_sem, feat_s, feat_r, inj_s, inj_r, up_s, up_r, side_s, side_r,
                 near_s, near_r, far_s, far_r, mail_s, mail_r, wide_s, wide_r):
    me = lax.axis_index("feat")
    side = lax.rem(me, 2)
    mine = lax.div(me, 2)
    partner = me + 1 - 2 * side
    lines = n // 2
    lined = [lax.rem(mine + d, lines) for d in range(lines)]
    before = [lax.rem(mine - d + lines, lines) for d in range(lines)]
    at_seq = lax.axis_index("seq")
    row_side = lax.rem(at_seq, 2)
    level = lax.div(at_seq, 2)
    levels = m // 2
    row_partner = at_seq + 1 - 2 * row_side

    toks, part = inj.shape
    width = n * part
    head_cols = w_q.shape[1]
    kv_cols = w_kv.shape[1] // 2
    kv_local = kv_cols // HEAD_DIM
    heads = head_cols // HEAD_DIM
    group = heads // kv_local
    span = part // CHUNKS
    half = toks // HALVES
    lanes = 128
    scale_all = float(toks * m * width)
    factor = math.log2(math.e) / math.sqrt(HEAD_DIM)
    f32, bf16 = jnp.float32, jnp.bfloat16

    loads = [
        pltpu.make_async_copy(inj_hbm, inj, load_sem.at[0]),
        pltpu.make_async_copy(warm_hbm, warm, load_sem.at[1]),
        pltpu.make_async_copy(wk_hbm, w_kv.at[:, pl.ds(0, kv_cols)], load_sem.at[2]),
        pltpu.make_async_copy(wv_hbm, w_kv.at[:, pl.ds(kv_cols, kv_cols)], load_sem.at[3]),
        pltpu.make_async_copy(wq_hbm, w_q, load_sem.at[4]),
        pltpu.make_async_copy(wo_hbm, w_o, load_sem.at[5]),
    ]
    for load in loads:
        load.start()

    barrier = pltpu.get_barrier_semaphore()
    for d in range(1, n):
        pl.semaphore_signal(barrier, inc=1, device_id={"feat": lax.rem(me + d, n)}, device_id_type=MESH)
    for d in range(1, m):
        pl.semaphore_signal(barrier, inc=1, device_id={"seq": lax.rem(at_seq + d, m)}, device_id_type=MESH)

    def columns(at, size):
        return pl.ds(pl.multiple_of(at * size, size), size)

    def blocks_of(ref_width):
        return ref_width // lanes

    def row_sums(partial):
        return jnp.broadcast_to(jnp.sum(partial.T, axis=0, keepdims=True), (8, toks))

    def by_token(total):
        scale = lax.rsqrt(total * (1.0 / width) + EPS)
        return jnp.broadcast_to(scale[:1], (lanes, toks)).T

    zero_tile = jnp.zeros((toks, lanes), f32)

    @pl.loop(0, blocks_of(part))
    def _(at):
        cols = columns(at, lanes)
        for j in range(ITERS):
            images[j, :, cols] = zero_tile
            residuals[j, :, cols] = zero_tile

    @pl.loop(0, blocks_of(head_cols + 2 * kv_cols))
    def _(at):
        cols = columns(at, lanes)
        for j in range(ITERS):
            proj[j, :, cols] = zero_tile

    for j in range(ITERS):
        coef[j] = jnp.full((8, lanes), 1.0 if j == 0 else 0.0, f32)
    for j in range(ITERS * ITERS):
        gram[j] = jnp.zeros((8, lanes), f32)
    scale_out[...] = jnp.ones((toks, lanes), f32)

    @pl.when(row_side == 0)
    def _():
        for slot in range(2):
            kv[slot, at_seq + 1] = jnp.zeros(kv.shape[2:], bf16)

    key_at = lax.broadcasted_iota(jnp.int32, (toks, 2 * toks), 1)
    query_at = lax.broadcasted_iota(jnp.int32, (toks, 2 * toks), 0) + row_side * toks
    bias[0] = jnp.where(key_at <= query_at, 0.0, -1e30).astype(f32)
    bias[1] = jnp.zeros((toks, 2 * toks), f32)

    loads[0].wait()
    loads[1].wait()

    def gather_copy(buffer, cols, sems, d):
        here = buffer.at[me, :, cols]
        target = partner if d == 0 else 2 * lined[d] + side
        return remote(here, here, sems[0], sems[1], "feat", target)

    def forward_copy(buffer, cols, sems, d):
        here = buffer.at[2 * before[d] + side, :, cols]
        return remote(here, here, sems[0], sems[1], "feat", partner)

    def gather_step(c, d):
        return gather_copy(tok, columns(c, span), (feat_s.at[c, d], feat_r.at[c, d]), d)

    def forward_step(c, d):
        at = lines - 1 + d
        return forward_copy(tok, columns(c, span), (feat_s.at[c, at], feat_r.at[c, at]), d)

    def inj_step(d):
        return gather_copy(tok_inj, pl.ds(0, part), (inj_s.at[d], inj_r.at[d]), d)

    def inj_forward(d):
        at = lines - 1 + d
        return forward_copy(tok_inj, pl.ds(0, part), (inj_s.at[at], inj_r.at[at]), d)

    def start_block(at, total):
        cols = columns(at, lanes)
        gain = gain_in[me, :, cols]
        base = inj[:, cols].astype(f32)
        first = warm[:, cols].astype(f32)
        out[:, cols] = first
        mixed = first + base
        tok[me, :, cols] = (mixed * gain).astype(bf16)
        tok_inj[me, :, cols] = (base * gain).astype(bf16)
        return total + mixed * mixed

    total = lax.fori_loop(0, blocks_of(part), start_block, zero_tile)
    mail_out[1] = row_sums(total)
    pl.semaphore_wait(barrier, n + m - 2)
    for c in range(CHUNKS):
        for d in range(1, lines):
            gather_step(c, d).start()
        gather_step(c, 0).start()
    for d in range(lines):
        inj_step(d).start()

    def feat_sum(which):
        copies = [
            remote(mail_out.at[which], mail.at[which, d], mail_s.at[which, d], mail_r.at[which, d],
                   "feat", lax.rem(me + d, n))
            for d in range(1, n)
        ]
        for copy in copies:
            copy.start()
        total = mail_out[which]
        for d, copy in enumerate(copies):
            copy.wait()
            total = total + mail[which, d + 1]
        return total

    def seq_sum(slot, value):
        wide_out[...] = value
        copies = [
            remote(wide_out, wide.at[slot, d], wide_s.at[slot, d], wide_r.at[slot, d],
                   "seq", lax.rem(at_seq + d, m))
            for d in range(1, m)
        ]
        for copy in copies:
            copy.start()
        for d, copy in enumerate(copies):
            copy.wait()
            value = value + wide[slot, d + 1]
        return value

    def settle(k, slot):
        scale_out[...] = by_token(feat_sum(0))

        def image_block(at, sums):
            cols = columns(at, lanes)
            image = held[:, cols] * scale_out[...] * gain_out[me, :, cols]
            residual = image - out[:, cols]
            images[k, :, cols] = image
            residuals[k, :, cols] = residual
            first = residuals[0, :, cols]
            pairs = [residual * residuals[j, :, cols] for j in range(ITERS)] + [first * first]
            return tuple(
                one + jnp.sum(pair.reshape(toks // 8, 8, lanes), axis=0) for one, pair in zip(sums, pairs)
            )

        zero = jnp.zeros((8, lanes), f32)
        sums = lax.fori_loop(0, blocks_of(part), image_block, (zero,) * (ITERS + 1))

        @pl.when(k > 0)
        def _():
            rows = [jnp.sum(one, axis=0, keepdims=True) for one in sums]
            mail_out[2] = jnp.concatenate(rows + [jnp.zeros((8 - len(rows), lanes), f32)], axis=0)
            total = seq_sum(slot, feat_sum(2))
            total = jnp.broadcast_to(jnp.sum(total, axis=1, keepdims=True), (8, lanes))
            values = [jnp.broadcast_to(total[j : j + 1], (8, lanes)) for j in range(ITERS + 1)]
            gram[0] = values[ITERS]
            for j in range(ITERS):
                gram[ITERS * k + j] = values[j]
                gram[ITERS * j + k] = values[j]
            system = []
            for i in range(ITERS):
                row = []
                for j in range(ITERS):
                    fixed = LAMBDA if i == j else 0.0
                    there = gram[ITERS * i + j] / scale_all + fixed
                    row.append(jnp.where(max(i, j) <= k, there, 1.0 if i == j else 0.0))
                system.append(row)
            goals = [jnp.where(i <= k, jnp.ones((8, lanes), f32), 0.0) for i in range(ITERS)]
            unscaled = solve_values(system, goals)
            whole = unscaled[0]
            for value in unscaled[1:]:
                whole = whole + value
            for j in range(ITERS):
                coef[j] = unscaled[j] / whole

        def mix_block(at, total):
            cols = columns(at, lanes)
            tiles = [jnp.broadcast_to(coef[j][:1], (toks, lanes)) for j in range(ITERS)]
            current = tiles[0] * images[0, :, cols]
            for j in range(1, ITERS):
                current = current + tiles[j] * images[j, :, cols]
            out[:, cols] = current
            mixed = current + inj[:, cols].astype(f32)
            return total + mixed * mixed

        mail_out[1] = row_sums(lax.fori_loop(0, blocks_of(part), mix_block, zero_tile))

    def kv_copy(slot, c, owner, sems, target):
        here = kv.at[slot, owner, pl.ds(c * half, half)]
        return remote(here, here, sems[0], sems[1], "seq", target)

    def up_step(slot, c, d, owner, target):
        return kv_copy(slot, c, owner, (up_s.at[c, d], up_r.at[slot, c, d]), target)

    def side_step(slot, c, k, owner):
        return kv_copy(slot, c, owner, (side_s.at[c, k], side_r.at[slot, c, k]), row_partner)

    def gathered(buffer):
        return jnp.concatenate([buffer[f] for f in range(n)], axis=1)

    def project(buffer, weights, cols):
        return jnp.dot(gathered(buffer), weights[:, cols], preferred_element_type=f32)

    def combined(cols, size):
        total = proj[ITERS - 1, :, cols]
        for j in range(ITERS - 1):
            total = total + jnp.broadcast_to(coef[j][:1, :1], (toks, size)) * proj[j, :, cols]
        return total

    def wide_scale(ref, size):
        return jnp.concatenate([ref[...]] * (size // lanes), axis=1)

    q_tile = span
    kv_tile = min(256, 2 * kv_cols)

    def attend(slot, k):
        owner = 2 * (level - k)
        which = jnp.minimum(k, 1)
        for e in range(kv_local):
            keys = kv[slot, pl.ds(owner, 2), :, e * HEAD_DIM : (e + 1) * HEAD_DIM].reshape(2 * toks, HEAD_DIM)
            values = kv[
                slot, pl.ds(owner, 2), :, kv_cols + e * HEAD_DIM : kv_cols + (e + 1) * HEAD_DIM
            ].reshape(2 * toks, HEAD_DIM)
            values = jnp.concatenate([values, jnp.ones((2 * toks, HEAD_DIM), bf16)], axis=1)
            asked = queries[e * group : (e + 1) * group].reshape(group * toks, HEAD_DIM)
            scores = lax.dot_general(asked, keys, (((1,), (1,)), ((), ())), preferred_element_type=f32)
            scores = (scores.reshape(group, toks, 2 * toks) + bias[which][None]).reshape(group * toks, 2 * toks)
            old = top[e]
            new = jnp.maximum(old, jnp.max(scores, axis=1, keepdims=True))
            top[e] = new
            both = jnp.concatenate([new] * (2 * toks // lanes), axis=1)
            weights = jnp.exp2((scores - both) * factor)
            fade = jnp.exp2((old - new) * factor)
            acc[e] = acc[e] * jnp.concatenate([fade, fade], axis=1) + jnp.dot(
                weights.astype(bf16), values, preferred_element_type=f32
            )

    def near_step(c, d):
        return remote(
            near_out.at[d, :, columns(c, span)], near.at[d, :, columns(c, span)],
            near_s.at[c, d], near_r.at[c, d], "feat", partner,
        )

    def far_step(c, d):
        return remote(
            outgoing.at[d, :, columns(c, span)], far.at[d, :, columns(c, span)],
            far_s.at[c, d], far_r.at[c, d], "feat", 2 * lined[d] + side,
        )

    def out_dot(target, c):
        cols = pl.ds(pl.multiple_of(target * part + c * span, span), span)
        return jnp.dot(attended[...], w_o[:, cols], preferred_element_type=f32)

    def pass_on(c):
        cols = columns(c, span)
        for d in range(1, lines):
            near_step(c, d).wait_recv()
            outgoing[d, :, cols] = (keep[d, :, cols] + near[d, :, cols].astype(f32)).astype(bf16)
            far_step(c, d).start()

    def own_dots(c):
        cols = columns(c, span)
        near_out[0, :, cols] = out_dot(2 * mine + 1 - side, c).astype(bf16)
        near_step(c, 0).start()
        keep[0, :, cols] = out_dot(me, c)

    def evaluate(it):
        slot = lax.rem(it, 2)
        k = jnp.maximum(it - 1, 0)
        scale_in[...] = by_token(feat_sum(1))

        @pl.when(it == 0)
        def _():
            loads[2].wait()
            loads[3].wait()

        @pl.when(it == 1)
        def _():
            for d in range(1, lines):
                inj_forward(d).wait()
            inj_step(0).wait()
            for d in range(1, lines):
                inj_step(d).wait_send()

            @pl.loop(0, 2 * kv_cols // kv_tile)
            def _(at):
                cols = columns(at, kv_tile)
                proj[ITERS - 1, :, cols] = project(tok_inj, w_kv, cols)

            @pl.loop(0, head_cols // q_tile)
            def _(at):
                put = pl.ds(pl.multiple_of(2 * kv_cols + at * q_tile, q_tile), q_tile)
                proj[ITERS - 1, :, put] = project(tok_inj, w_q, columns(at, q_tile))

        @pl.loop(0, CHUNKS)
        def _(c):
            for d in range(1, lines):
                gather_step(c, d).wait_recv()
                forward_step(c, d).start()

        @pl.loop(0, CHUNKS)
        def _(c):
            gather_step(c, 0).wait()
            for d in range(1, lines):
                forward_step(c, d).wait()
                gather_step(c, d).wait_send()

        @pl.loop(0, 2 * kv_cols // kv_tile)
        def _(at):
            cols = columns(at, kv_tile)
            proj[k, :, cols] = project(tok, w_kv, cols) * wide_scale(scale_out, kv_tile)
            kv[slot, at_seq, :, cols] = (combined(cols, kv_tile) * wide_scale(scale_in, kv_tile)).astype(bf16)

        for c in range(HALVES):
            @pl.when(row_side == 0)
            def _():
                side_step(slot, c, 0, at_seq).start()

            for d in range(levels - 1, 0, -1):
                @pl.when(level + d < levels)
                def _():
                    up_step(slot, c, d, at_seq, at_seq + 2 * d).start()

        @pl.when(it == 0)
        def _():
            loads[4].wait()

        @pl.loop(0, head_cols // q_tile)
        def _(at):
            put = pl.ds(pl.multiple_of(2 * kv_cols + at * q_tile, q_tile), q_tile)
            proj[k, :, put] = project(tok, w_q, columns(at, q_tile)) * wide_scale(scale_out, q_tile)
            asked = (combined(put, q_tile) * wide_scale(scale_in, q_tile)).astype(bf16)
            for h in range(q_tile // HEAD_DIM):
                queries[at * (q_tile // HEAD_DIM) + h] = asked[:, h * HEAD_DIM : (h + 1) * HEAD_DIM]

        for e in range(kv_local):
            top[e] = jnp.full(top.shape[1:], -1e30, f32)
            acc[e] = jnp.zeros(acc.shape[1:], f32)

        @pl.loop(0, level + 1)
        def _(k):
            @pl.when(k + 1 <= level)
            def _():
                owner = at_seq - 2 * (k + 1)
                for c in range(HALVES):
                    up_step(slot, c, k + 1, owner, owner).wait_recv()
                    side_step(slot, c, k + 1, owner).start()

            @pl.when(k + row_side > 0)
            def _():
                for c in range(HALVES):
                    side_step(slot, c, k, row_partner - 2 * k).wait_recv()

            attend(slot, k)

        for e in range(kv_local):
            for g in range(group):
                rows = slice(g * toks, (g + 1) * toks)
                at = (e * group + g) * HEAD_DIM
                attended[:, at : at + HEAD_DIM] = (
                    acc[e, rows, :HEAD_DIM] / acc[e, rows, HEAD_DIM:]
                ).astype(bf16)

        @pl.when(it == 0)
        def _():
            loads[5].wait()
            for d in range(1, lines):
                inj_step(d).wait_recv()
                inj_forward(d).start()

        @pl.loop(0, CHUNKS)
        def _(c):
            cols = columns(c, span)
            for d in range(1, lines):
                near_out[d, :, cols] = out_dot(2 * lined[d] + 1 - side, c).astype(bf16)
                near_step(c, d).start()
                keep[d, :, cols] = out_dot(2 * lined[d] + side, c)

            @pl.when(c > 0)
            def _():
                pass_on(c - 1)

        own_dots(0)
        pass_on(CHUNKS - 1)

        @pl.loop(1, CHUNKS)
        def _(c):
            own_dots(c)

        def finish(c, total):
            near_step(c, 0).wait()
            for d in range(1, lines):
                near_step(c, d).wait_send()
                far_step(c, d).wait()
            for at in range(span // lanes):
                cols = pl.ds(pl.multiple_of(c * span + at * lanes, lanes), lanes)
                update = keep[0, :, cols] + near[0, :, cols].astype(f32)
                for d in range(1, lines):
                    update = update + far[d, :, cols].astype(f32)
                summed = out[:, cols] + inj[:, cols].astype(f32) + update
                held[:, cols] = summed
                tok[me, :, cols] = (summed * gain_out[me, :, cols] * gain_in[me, :, cols]).astype(bf16)
                total = total + summed * summed

            @pl.when(it + 1 < ITERS)
            def _():
                for d in range(1, lines):
                    gather_step(c, d).start()
                gather_step(c, 0).start()

            return total

        mail_out[0] = row_sums(lax.fori_loop(0, CHUNKS, finish, zero_tile))

        for c in range(HALVES):
            @pl.when(row_side == 0)
            def _():
                side_step(slot, c, 0, at_seq).wait_send()

            for d in range(levels - 1, 0, -1):
                @pl.when(level + d < levels)
                def _():
                    up_step(slot, c, d, at_seq, at_seq + 2 * d).wait_send()

        @pl.loop(1, level + 1)
        def _(k):
            for c in range(HALVES):
                side_step(slot, c, k, at_seq - 2 * k).wait_send()

    @pl.loop(0, ITERS + 1)
    def _(it):
        @pl.when(it > 0)
        def _():
            settle(it - 1, lax.rem(it, 2))

        @pl.when(it < ITERS)
        def _():
            evaluate(it)


def on_device(injection, warm_start, gain_in, gain_out, w_query, w_key, w_value, w_out):
    n, m = lax.axis_size("feat"), lax.axis_size("seq")
    toks, part = injection.shape
    head_cols, kv_cols = w_query.shape[1], w_key.shape[1]
    kv_local = kv_cols // HEAD_DIM
    group = HEADS // KV_HEADS
    lines = n // 2
    f32, bf16 = jnp.float32, jnp.bfloat16
    vmem, dma = pltpu.VMEM, pltpu.SemaphoreType.DMA
    lanes = 128
    scratch = [
        vmem((n, toks, part), bf16), vmem((n, toks, part), bf16),
        vmem((w_key.shape[0], 2 * kv_cols), bf16), vmem(w_query.shape, bf16), vmem(w_out.shape, bf16),
        vmem((toks, part), bf16), vmem((toks, part), bf16),
        vmem((ITERS, toks, part), f32), vmem((ITERS, toks, part), f32), vmem((toks, part), f32),
        vmem((ITERS, toks, head_cols + 2 * kv_cols), f32),
        vmem((head_cols // HEAD_DIM, toks, HEAD_DIM), bf16),
        vmem((2, m, toks, 2 * kv_cols), bf16),
        vmem((kv_local, group * toks, 2 * HEAD_DIM), f32), vmem((kv_local, group * toks, lanes), f32),
        vmem((2, toks, 2 * toks), f32), vmem((toks, head_cols), bf16),
        vmem((lines, toks, part), f32),
        vmem((lines, toks, part), bf16), vmem((lines, toks, part), bf16),
        vmem((lines, toks, part), bf16), vmem((lines, toks, part), bf16),
        vmem((ITERS, 8, lanes), f32), vmem((ITERS * ITERS, 8, lanes), f32),
        vmem((toks, lanes), f32), vmem((toks, lanes), f32),
        vmem((3, 8, toks), f32), vmem((3, n, 8, toks), f32),
        vmem((8, lanes), f32), vmem((2, m, 8, lanes), f32),
        dma((6,)), dma((CHUNKS, n)), dma((CHUNKS, n)), dma((n,)), dma((n,)),
        dma((HALVES, m // 2)), dma((2, HALVES, m // 2)), dma((HALVES, m // 2)), dma((2, HALVES, m // 2)),
        dma((CHUNKS, lines)), dma((CHUNKS, lines)), dma((CHUNKS, lines)), dma((CHUNKS, lines)),
        dma((3, n)), dma((3, n)), dma((2, m)), dma((2, m)),
    ]
    return pl.pallas_call(
        functools.partial(whole_kernel, n, m),
        out_shape=jax.ShapeDtypeStruct((toks, part), f32),
        in_specs=[ANY, ANY, VMEM, VMEM, ANY, ANY, ANY, ANY],
        out_specs=VMEM,
        scratch_shapes=scratch,
        compiler_params=pltpu.CompilerParams(
            collective_id=0, has_side_effects=True, vmem_limit_bytes=63 * 1024 * 1024
        ),
    )(
        injection, warm_start, gain_in.reshape(n, 1, part), gain_out.reshape(n, 1, part),
        w_query, w_key, w_value, w_out,
    )


def solution(mesh):
    in_specs = (
        P("seq", "feat"),
        P("seq", "feat"),
        P(),
        P(),
        P(None, "feat"),
        P(None, "feat"),
        P(None, "feat"),
        P("feat", None),
    )
    out_specs = P("seq", "feat")
    return jax.shard_map(
        on_device, mesh=mesh, in_specs=in_specs, out_specs=out_specs, check_vma=False
    )
```

```python
import functools
import math

import jax
import jax.numpy as jnp
from jax import lax
from jax.experimental import pallas as pl
from jax.experimental.pallas import tpu as pltpu
from jax.sharding import PartitionSpec as P

HEADS = 40
KV_HEADS = 8
HEAD_DIM = 128
ITERS = 4

EPS = 1e-06
LAMBDA = 0.03
CHUNKS = 5
HALVES = 4
EARLY = 3
ROWS = 7
WARM = ITERS
INJ = ITERS + 1
MESH = pl.DeviceIdType.MESH
VMEM = pl.BlockSpec(memory_space=pltpu.VMEM)
ANY = pl.BlockSpec(memory_space=pl.ANY)


def remote(src, dst, send_sem, recv_sem, axis, target):
    return pltpu.make_async_remote_copy(
        src_ref=src, dst_ref=dst, send_sem=send_sem, recv_sem=recv_sem,
        device_id={axis: target}, device_id_type=MESH,
    )


def solve_values(rows, values):
    size = len(values)
    rows = [list(row) for row in rows]
    values = list(values)
    for pivot in range(size):
        for below in range(pivot + 1, size):
            ratio = rows[below][pivot] / rows[pivot][pivot]
            for at in range(pivot, size):
                rows[below][at] = rows[below][at] - ratio * rows[pivot][at]
            values[below] = values[below] - ratio * values[pivot]
    result = [None] * size
    for pivot in reversed(range(size)):
        running = values[pivot]
        for later in range(pivot + 1, size):
            running = running - rows[pivot][later] * result[later]
        result[pivot] = running / rows[pivot][pivot]
    return result


def whole_kernel(n, m, inj_hbm, warm_hbm, gain_in, gain_out, wq_hbm, wk_hbm, wv_hbm, wo_hbm, out,
                 tok, tok_inj, w_kv, w_q, w_o, inj, warm, images, held, proj, queries, kv,
                 acc, top, bias, attended, keep, near_out, near, outgoing, far, coef, gram, dots, totals, mixing, sums,
                 scale_out, scale_in, mail_out, mail, wide_out, wide,
                 load_sem, feat_s, feat_r, inj_s, inj_r, up_s, up_r, side_s, side_r,
                 near_s, near_r, far_s, far_r, mail_s, mail_r, wide_s, wide_r):
    me = lax.axis_index("feat")
    side = lax.rem(me, 2)
    mine = lax.div(me, 2)
    partner = me + 1 - 2 * side
    lines = n // 2
    lined = [lax.rem(mine + d, lines) for d in range(lines)]
    before = [lax.rem(mine - d + lines, lines) for d in range(lines)]
    at_seq = lax.axis_index("seq")
    row_side = lax.rem(at_seq, 2)
    level = lax.div(at_seq, 2)
    levels = m // 2
    row_partner = at_seq + 1 - 2 * row_side

    toks, part = inj.shape
    width = n * part
    head_cols = w_q.shape[1]
    kv_cols = w_kv.shape[1] // 2
    kv_local = kv_cols // HEAD_DIM
    heads = head_cols // HEAD_DIM
    group = heads // kv_local
    span = part // CHUNKS
    half = toks // HALVES
    lanes = 128
    scale_all = float(toks * m * width)
    factor = math.log2(math.e) / math.sqrt(HEAD_DIM)
    f32, bf16 = jnp.float32, jnp.bfloat16

    loads = [
        pltpu.make_async_copy(inj_hbm, inj, load_sem.at[0]),
        pltpu.make_async_copy(warm_hbm, warm, load_sem.at[1]),
        pltpu.make_async_copy(wk_hbm, w_kv.at[:, pl.ds(0, kv_cols)], load_sem.at[2]),
        pltpu.make_async_copy(wv_hbm, w_kv.at[:, pl.ds(kv_cols, kv_cols)], load_sem.at[3]),
        pltpu.make_async_copy(wq_hbm, w_q, load_sem.at[4]),
        pltpu.make_async_copy(wo_hbm, w_o, load_sem.at[5]),
    ]
    for load in loads:
        load.start()

    barrier = pltpu.get_barrier_semaphore()
    for d in range(1, n):
        pl.semaphore_signal(barrier, inc=1, device_id={"feat": lax.rem(me + d, n)}, device_id_type=MESH)
    for d in range(1, m):
        pl.semaphore_signal(barrier, inc=1, device_id={"seq": lax.rem(at_seq + d, m)}, device_id_type=MESH)

    def columns(at, size):
        return pl.ds(pl.multiple_of(at * size, size), size)

    def blocks_of(ref_width):
        return ref_width // lanes

    def row_sums(partials):
        rows = [jnp.sum(partial.T, axis=0, keepdims=True) for partial in partials]
        return jnp.concatenate(rows + [jnp.zeros((8 - len(rows), toks), f32)], axis=0)

    def inverse_rms(total):
        return lax.rsqrt(total * (1.0 / width) + EPS)

    def by_token(row):
        return jnp.broadcast_to(row[:1], (lanes, toks)).T

    def everywhere(row):
        return jnp.broadcast_to(row, (8, row.shape[1]))

    zero_tile = jnp.zeros((toks, lanes), f32)

    @pl.loop(0, blocks_of(part))
    def _(at):
        cols = columns(at, lanes)
        for j in range(ITERS):
            images[j, :, cols] = zero_tile

    @pl.loop(0, blocks_of(head_cols + 2 * kv_cols))
    def _(at):
        cols = columns(at, lanes)
        for j in range(ITERS):
            proj[j, :, cols] = zero_tile

    small_zero = jnp.zeros((8, lanes), f32)
    for j in range(ITERS):
        coef[j] = jnp.full((8, lanes), 1.0 if j == 0 else 0.0, f32)
    for j in range(ITERS * ITERS):
        gram[j] = small_zero
    for j in range((WARM + 1) * (WARM + 1)):
        totals[j] = small_zero
    for j in range(ITERS * (WARM + 1)):
        mixing[j] = small_zero
    for j in range((INJ + 1) * (INJ + 1)):
        dots[j] = jnp.zeros((8, toks), f32)
    scale_out[...] = jnp.ones((toks, lanes), f32)

    @pl.when(row_side == 0)
    def _():
        for slot in range(2):
            kv[slot, at_seq + 1] = jnp.zeros(kv.shape[2:], bf16)

    key_at = lax.broadcasted_iota(jnp.int32, (toks, 2 * toks), 1)
    query_at = lax.broadcasted_iota(jnp.int32, (toks, 2 * toks), 0) + row_side * toks
    bias[0] = jnp.where(key_at <= query_at, 0.0, -1e30).astype(f32)
    bias[1] = jnp.zeros((toks, 2 * toks), f32)

    loads[0].wait()
    loads[1].wait()

    def gather_copy(buffer, cols, sems, d):
        here = buffer.at[me, :, cols]
        target = partner if d == 0 else 2 * lined[d] + side
        return remote(here, here, sems[0], sems[1], "feat", target)

    def forward_copy(buffer, cols, sems, d):
        here = buffer.at[2 * before[d] + side, :, cols]
        return remote(here, here, sems[0], sems[1], "feat", partner)

    def gather_step(c, d):
        return gather_copy(tok, columns(c, span), (feat_s.at[c, d], feat_r.at[c, d]), d)

    def forward_step(c, d):
        at = lines - 1 + d
        return forward_copy(tok, columns(c, span), (feat_s.at[c, at], feat_r.at[c, at]), d)

    def inj_step(d):
        return gather_copy(tok_inj, pl.ds(0, part), (inj_s.at[d], inj_r.at[d]), d)

    def inj_forward(d):
        at = lines - 1 + d
        return forward_copy(tok_inj, pl.ds(0, part), (inj_s.at[at], inj_r.at[at]), d)

    def start_block(at, totals_now):
        cols = columns(at, lanes)
        gain = gain_in[me, :, cols]
        base = inj[:, cols].astype(f32)
        first = warm[:, cols].astype(f32)
        out[:, cols] = first
        mixed = first + base
        tok[me, :, cols] = (mixed * gain).astype(bf16)
        tok_inj[me, :, cols] = (base * gain).astype(bf16)
        pairs = (first * first, base * base, mixed * mixed)
        return tuple(total + pair for total, pair in zip(totals_now, pairs))

    mail_out[1] = row_sums(lax.fori_loop(0, blocks_of(part), start_block, (zero_tile,) * 3))

    def mail_copies(which):
        return [
            remote(mail_out.at[which], mail.at[which, d], mail_s.at[which, d], mail_r.at[which, d],
                   "feat", lax.rem(me + d, n))
            for d in range(1, n)
        ]

    def mail_start(which):
        for copy in mail_copies(which):
            copy.start()

    def mail_total(which):
        total = mail_out[which]
        for d, copy in enumerate(mail_copies(which)):
            copy.wait()
            total = total + mail[which, d + 1]
        return total

    def wide_copies(slot):
        return [
            remote(wide_out, wide.at[slot, d], wide_s.at[slot, d], wide_r.at[slot, d],
                   "seq", lax.rem(at_seq + d, m))
            for d in range(1, m)
        ]

    def wide_total(slot):
        total = wide_out[...]
        for d, copy in enumerate(wide_copies(slot)):
            copy.wait()
            total = total + wide[slot, d + 1]
        return total

    def start_gather(c):
        for d in range(1, lines):
            gather_step(c, d).start()
        gather_step(c, 0).start()

    def relay(c):
        for d in range(1, lines):
            gather_step(c, d).wait_recv()
            forward_step(c, d).start()

    pl.semaphore_wait(barrier, n + m - 2)
    mail_start(1)
    for c in range(CHUNKS):
        start_gather(c)

    def dot_at(i, j):
        return dots[(INJ + 1) * i + j]

    def total_at(i, j):
        return totals[(WARM + 1) * i + j]

    def settle(k, slot, more):
        total = mail_total(0)
        rate = inverse_rms(total[:1])
        scale_out[...] = by_token(rate)
        for at, j in enumerate(list(range(ITERS - 1)) + [WARM, INJ]):
            value = everywhere(total[at + 1 : at + 2] * rate)
            dots[(INJ + 1) * k + j] = value
            dots[(INJ + 1) * j + k] = value
        dots[(INJ + 2) * k] = everywhere(total[ROWS - 1 : ROWS] * rate * rate)
        for j in range(WARM + 1):
            before_now = jnp.where(k == 0, 1.0 if j == WARM else 0.0, coef[j] if j < WARM else 0.0)
            mixing[(WARM + 1) * k + j] = jnp.where(k == j, 1.0, 0.0) - before_now * jnp.ones((8, lanes), f32)

        @pl.when(k > 0)
        def _():
            rows = [dots[(INJ + 1) * k + j][:1] for j in range(WARM + 1)]
            rows = rows + [dot_at(0, 0)[:1], dot_at(0, WARM)[:1], dot_at(WARM, WARM)[:1]]
            wide_out[...] = jnp.concatenate(rows, axis=0)
            for copy in wide_copies(slot):
                copy.start()

        @pl.when(more)
        def _():
            for c in range(EARLY):
                relay(c)

        @pl.when(k > 0)
        def _():
            total = jnp.broadcast_to(jnp.sum(wide_total(slot), axis=1, keepdims=True), (8, lanes))
            values = [jnp.broadcast_to(total[j : j + 1], (8, lanes)) for j in range(8)]
            for j in range(WARM + 1):
                totals[(WARM + 1) * k + j] = values[j]
                totals[(WARM + 1) * j + k] = values[j]
            totals[0] = values[WARM + 1]
            totals[WARM] = values[WARM + 2]
            totals[(WARM + 1) * WARM] = values[WARM + 2]
            totals[(WARM + 1) * WARM + WARM] = values[WARM + 3]

            def product(i, j):
                run = small_zero
                for a in range(WARM + 1):
                    inner = small_zero
                    for b in range(WARM + 1):
                        inner = inner + total_at(a, b) * mixing[(WARM + 1) * j + b]
                    run = run + mixing[(WARM + 1) * i + a] * inner
                return run

            gram[0] = product(0, 0)
            for j in range(ITERS):
                value = product(j, k)
                gram[ITERS * k + j] = value
                gram[ITERS * j + k] = value
            system = []
            for i in range(ITERS):
                row = []
                for j in range(ITERS):
                    fixed = LAMBDA if i == j else 0.0
                    there = gram[ITERS * i + j] / scale_all + fixed
                    row.append(jnp.where(max(i, j) <= k, there, 1.0 if i == j else 0.0))
                system.append(row)
            goals = [jnp.where(i <= k, jnp.ones((8, lanes), f32), 0.0) for i in range(ITERS)]
            unscaled = solve_values(system, goals)
            whole = unscaled[0]
            for value in unscaled[1:]:
                whole = whole + value
            for j in range(ITERS):
                coef[j] = unscaled[j] / whole

        parts_now = [jnp.broadcast_to(coef[j][:, :1], (8, toks)) for j in range(ITERS)]
        square = dot_at(INJ, INJ)
        for i in range(ITERS):
            inner = 2.0 * dot_at(i, INJ)
            for j in range(ITERS):
                inner = inner + parts_now[j] * dot_at(i, j)
            square = square + parts_now[i] * inner
        scale_in[...] = by_token(inverse_rms(jnp.maximum(square, 0.0)))

    def remix(k):
        @pl.loop(0, blocks_of(part))
        def _(at):
            cols = columns(at, lanes)
            images[k, :, cols] = held[:, cols] * scale_out[...] * gain_out[me, :, cols]
            current = coef[0][:1] * images[0, :, cols]
            for j in range(1, ITERS):
                current = current + coef[j][:1] * images[j, :, cols]
            out[:, cols] = current

    def kv_copy(slot, c, owner, sems, target):
        here = kv.at[slot, owner, pl.ds(c * half, half)]
        return remote(here, here, sems[0], sems[1], "seq", target)

    def up_step(slot, c, k, owner, target):
        return kv_copy(slot, c, owner, (up_s.at[c, k], up_r.at[slot, c, k]), target)

    def side_step(slot, c, k, owner):
        return kv_copy(slot, c, owner, (side_s.at[c, k], side_r.at[slot, c, k]), row_partner)

    def gathered(buffer):
        return jnp.concatenate([buffer[f] for f in range(n)], axis=1)

    def project(buffer, weights, cols):
        return jnp.dot(gathered(buffer), weights[:, cols], preferred_element_type=f32)

    def combined(cols, size):
        total = proj[ITERS - 1, :, cols]
        for j in range(ITERS - 1):
            total = total + jnp.broadcast_to(coef[j][:1, :1], (toks, size)) * proj[j, :, cols]
        return total

    def wide_scale(ref, size):
        return jnp.concatenate([ref[...]] * (size // lanes), axis=1)

    q_tile = span
    kv_tile = min(256, 2 * kv_cols)

    def attend(slot, k):
        owner = 2 * (level - k)
        which = jnp.minimum(k, 1)
        for e in range(kv_local):
            keys = kv[slot, pl.ds(owner, 2), :, e * HEAD_DIM : (e + 1) * HEAD_DIM].reshape(2 * toks, HEAD_DIM)
            values = kv[
                slot, pl.ds(owner, 2), :, kv_cols + e * HEAD_DIM : kv_cols + (e + 1) * HEAD_DIM
            ].reshape(2 * toks, HEAD_DIM)
            values = jnp.concatenate([values, jnp.ones((2 * toks, HEAD_DIM), bf16)], axis=1)
            asked = queries[e * group : (e + 1) * group].reshape(group * toks, HEAD_DIM)
            scores = lax.dot_general(asked, keys, (((1,), (1,)), ((), ())), preferred_element_type=f32)
            scores = (scores.reshape(group, toks, 2 * toks) + bias[which][None]).reshape(group * toks, 2 * toks)
            old = top[e]
            new = jnp.maximum(old, jnp.max(scores, axis=1, keepdims=True))
            top[e] = new
            both = jnp.concatenate([new] * (2 * toks // lanes), axis=1)
            weights = jnp.exp2((scores - both) * factor)
            fade = jnp.exp2((old - new) * factor)
            acc[e] = acc[e] * jnp.concatenate([fade, fade], axis=1) + jnp.dot(
                weights.astype(bf16), values, preferred_element_type=f32
            )

    def near_step(c, d):
        return remote(
            near_out.at[d, :, columns(c, span)], near.at[d, :, columns(c, span)],
            near_s.at[c, d], near_r.at[c, d], "feat", partner,
        )

    def far_step(c, d):
        return remote(
            outgoing.at[d, :, columns(c, span)], far.at[d, :, columns(c, span)],
            far_s.at[c, d], far_r.at[c, d], "feat", 2 * lined[d] + side,
        )

    def out_dot(target, c):
        cols = pl.ds(pl.multiple_of(target * part + c * span, span), span)
        return jnp.dot(attended[...], w_o[:, cols], preferred_element_type=f32)

    def pass_on(c):
        cols = columns(c, span)
        for d in range(1, lines):
            near_step(c, d).wait_recv()
            outgoing[d, :, cols] = (keep[d, :, cols] + near[d, :, cols].astype(f32)).astype(bf16)
            far_step(c, d).start()

    def own_dots(c):
        cols = columns(c, span)
        near_out[0, :, cols] = out_dot(2 * mine + 1 - side, c).astype(bf16)
        near_step(c, 0).start()
        keep[0, :, cols] = out_dot(me, c)

    def arrive(slot, k):
        @pl.when(k <= level)
        def _():
            owner = at_seq - 2 * k
            for c in range(HALVES):
                up_step(slot, c, k - 1, owner, owner).wait_recv()

                @pl.when(level + 1 < levels)
                def _():
                    up_step(slot, c, k, owner, at_seq + 2).start()

                side_step(slot, c, k, owner).start()

    def send_keys(it):
        slot = lax.rem(it, 2)
        k = jnp.maximum(it - 1, 0)

        @pl.when(it == 0)
        def _():
            total = mail_total(1)
            dots[(INJ + 1) * WARM + WARM] = everywhere(total[:1])
            dots[(INJ + 1) * INJ + INJ] = everywhere(total[1:2])
            scale_in[...] = by_token(inverse_rms(total[2:3]))
            loads[2].wait()
            loads[3].wait()

        @pl.when(it == 1)
        def _():
            for d in range(1, lines):
                inj_forward(d).wait()
            inj_step(0).wait()
            for d in range(1, lines):
                inj_step(d).wait_send()

            @pl.loop(0, 2 * kv_cols // kv_tile)
            def _(at):
                cols = columns(at, kv_tile)
                proj[ITERS - 1, :, cols] = project(tok_inj, w_kv, cols)

            @pl.loop(0, head_cols // q_tile)
            def _(at):
                put = pl.ds(pl.multiple_of(2 * kv_cols + at * q_tile, q_tile), q_tile)
                proj[ITERS - 1, :, put] = project(tok_inj, w_q, columns(at, q_tile))

        @pl.loop(jnp.where(it > 0, EARLY, 0), CHUNKS)
        def _(c):
            relay(c)

        @pl.loop(0, CHUNKS)
        def _(c):
            gather_step(c, 0).wait()
            for d in range(1, lines):
                forward_step(c, d).wait()
                gather_step(c, d).wait_send()

        @pl.loop(0, 2 * kv_cols // kv_tile)
        def _(at):
            cols = columns(at, kv_tile)
            proj[k, :, cols] = project(tok, w_kv, cols) * wide_scale(scale_out, kv_tile)
            kv[slot, at_seq, :, cols] = (combined(cols, kv_tile) * wide_scale(scale_in, kv_tile)).astype(bf16)

        for c in range(HALVES):
            @pl.when(row_side == 0)
            def _():
                side_step(slot, c, 0, at_seq).start()

            @pl.when(level + 1 < levels)
            def _():
                up_step(slot, c, 0, at_seq, at_seq + 2).start()

        @pl.when(it == 0)
        def _():
            loads[4].wait()
            for d in range(lines):
                inj_step(d).start()

        @pl.loop(0, head_cols // q_tile)
        def _(at):
            put = pl.ds(pl.multiple_of(2 * kv_cols + at * q_tile, q_tile), q_tile)
            proj[k, :, put] = project(tok, w_q, columns(at, q_tile)) * wide_scale(scale_out, q_tile)
            asked = (combined(put, q_tile) * wide_scale(scale_in, q_tile)).astype(bf16)
            for h in range(q_tile // HEAD_DIM):
                queries[at * (q_tile // HEAD_DIM) + h] = asked[:, h * HEAD_DIM : (h + 1) * HEAD_DIM]

        for e in range(kv_local):
            top[e] = jnp.full(top.shape[1:], -1e30, f32)
            acc[e] = jnp.zeros(acc.shape[1:], f32)

        arrive(slot, 1)

    def finish_layer(it):
        slot = lax.rem(it, 2)

        @pl.loop(0, level + 1)
        def _(k):
            @pl.when(k > 0)
            def _():
                arrive(slot, k + 1)

            @pl.when(k + row_side > 0)
            def _():
                for c in range(HALVES):
                    side_step(slot, c, k, row_partner - 2 * k).wait_recv()

            attend(slot, k)

        for e in range(kv_local):
            for g in range(group):
                rows = slice(g * toks, (g + 1) * toks)
                at = (e * group + g) * HEAD_DIM
                attended[:, at : at + HEAD_DIM] = (
                    acc[e, rows, :HEAD_DIM] / acc[e, rows, HEAD_DIM:]
                ).astype(bf16)

        @pl.when(it == 0)
        def _():
            loads[5].wait()
            for d in range(1, lines):
                inj_step(d).wait_recv()
                inj_forward(d).start()

        @pl.loop(0, CHUNKS)
        def _(c):
            cols = columns(c, span)
            for d in range(1, lines):
                near_out[d, :, cols] = out_dot(2 * lined[d] + 1 - side, c).astype(bf16)
                near_step(c, d).start()
                keep[d, :, cols] = out_dot(2 * lined[d] + side, c)

            @pl.when(c > 0)
            def _():
                pass_on(c - 1)

        own_dots(0)
        pass_on(CHUNKS - 1)

        @pl.loop(1, CHUNKS)
        def _(c):
            own_dots(c)

        for at in range(ROWS):
            sums[at] = zero_tile

        @pl.loop(0, CHUNKS)
        def _(c):
            near_step(c, 0).wait()
            for d in range(1, lines):
                near_step(c, d).wait_send()
                far_step(c, d).wait()
            for at in range(span // lanes):
                cols = pl.ds(pl.multiple_of(c * span + at * lanes, lanes), lanes)
                update = keep[0, :, cols] + near[0, :, cols].astype(f32)
                for d in range(1, lines):
                    update = update + far[d, :, cols].astype(f32)
                base = inj[:, cols].astype(f32)
                summed = out[:, cols] + base + update
                held[:, cols] = summed
                scaled = summed * gain_out[me, :, cols]
                tok[me, :, cols] = (scaled * gain_in[me, :, cols]).astype(bf16)
                others = [images[j, :, cols] for j in range(ITERS - 1)]
                others = others + [warm[:, cols].astype(f32), base, scaled]
                sums[0] += summed * summed
                for row, other in enumerate(others):
                    sums[row + 1] += scaled * other

            @pl.when((it + 1 < ITERS) & (c == CHUNKS - 2))
            def _():
                start_gather(0)

        mail_out[0] = row_sums([sums[at] for at in range(ROWS)])
        mail_start(0)

        @pl.when(it + 1 < ITERS)
        def _():
            for c in range(1, CHUNKS):
                start_gather(c)

        for c in range(HALVES):
            @pl.when(row_side == 0)
            def _():
                side_step(slot, c, 0, at_seq).wait_send()

            @pl.when(level + 1 < levels)
            def _():
                up_step(slot, c, 0, at_seq, at_seq + 2).wait_send()

        @pl.loop(1, level + 1)
        def _(k):
            for c in range(HALVES):
                side_step(slot, c, k, at_seq - 2 * k).wait_send()

                @pl.when(level + 1 < levels)
                def _():
                    up_step(slot, c, k, at_seq - 2 * k, at_seq + 2).wait_send()

    @pl.loop(0, ITERS + 1)
    def _(it):
        @pl.when(it > 0)
        def _():
            settle(it - 1, lax.rem(it, 2), it < ITERS)

        @pl.when(it < ITERS)
        def _():
            send_keys(it)

        @pl.when(it > 0)
        def _():
            remix(it - 1)

        @pl.when(it < ITERS)
        def _():
            finish_layer(it)


def on_device(injection, warm_start, gain_in, gain_out, w_query, w_key, w_value, w_out):
    n, m = lax.axis_size("feat"), lax.axis_size("seq")
    toks, part = injection.shape
    head_cols, kv_cols = w_query.shape[1], w_key.shape[1]
    kv_local = kv_cols // HEAD_DIM
    group = HEADS // KV_HEADS
    lines = n // 2
    f32, bf16 = jnp.float32, jnp.bfloat16
    vmem, dma = pltpu.VMEM, pltpu.SemaphoreType.DMA
    lanes = 128
    scratch = [
        vmem((n, toks, part), bf16), vmem((n, toks, part), bf16),
        vmem((w_key.shape[0], 2 * kv_cols), bf16), vmem(w_query.shape, bf16), vmem(w_out.shape, bf16),
        vmem((toks, part), bf16), vmem((toks, part), bf16),
        vmem((ITERS, toks, part), f32), vmem((toks, part), f32),
        vmem((ITERS, toks, head_cols + 2 * kv_cols), f32),
        vmem((head_cols // HEAD_DIM, toks, HEAD_DIM), bf16),
        vmem((2, m, toks, 2 * kv_cols), bf16),
        vmem((kv_local, group * toks, 2 * HEAD_DIM), f32), vmem((kv_local, group * toks, lanes), f32),
        vmem((2, toks, 2 * toks), f32), vmem((toks, head_cols), bf16),
        vmem((lines, toks, part), f32),
        vmem((lines, toks, part), bf16), vmem((lines, toks, part), bf16),
        vmem((lines, toks, part), bf16), vmem((lines, toks, part), bf16),
        vmem((ITERS, 8, lanes), f32), vmem((ITERS * ITERS, 8, lanes), f32),
        vmem(((INJ + 1) * (INJ + 1), 8, toks), f32), vmem(((WARM + 1) * (WARM + 1), 8, lanes), f32),
        vmem((ITERS * (WARM + 1), 8, lanes), f32), vmem((ROWS, toks, lanes), f32),
        vmem((toks, lanes), f32), vmem((toks, lanes), f32),
        vmem((3, 8, toks), f32), vmem((3, n, 8, toks), f32),
        vmem((8, lanes), f32), vmem((2, m, 8, lanes), f32),
        dma((6,)), dma((CHUNKS, n)), dma((CHUNKS, n)), dma((n,)), dma((n,)),
        dma((HALVES, m // 2)), dma((2, HALVES, m // 2)), dma((HALVES, m // 2)), dma((2, HALVES, m // 2)),
        dma((CHUNKS, lines)), dma((CHUNKS, lines)), dma((CHUNKS, lines)), dma((CHUNKS, lines)),
        dma((3, n)), dma((3, n)), dma((2, m)), dma((2, m)),
    ]
    return pl.pallas_call(
        functools.partial(whole_kernel, n, m),
        out_shape=jax.ShapeDtypeStruct((toks, part), f32),
        in_specs=[ANY, ANY, VMEM, VMEM, ANY, ANY, ANY, ANY],
        out_specs=VMEM,
        scratch_shapes=scratch,
        compiler_params=pltpu.CompilerParams(
            collective_id=0, has_side_effects=True, vmem_limit_bytes=63 * 1024 * 1024
        ),
    )(
        injection, warm_start, gain_in.reshape(n, 1, part), gain_out.reshape(n, 1, part),
        w_query, w_key, w_value, w_out,
    )


def solution(mesh):
    in_specs = (
        P("seq", "feat"),
        P("seq", "feat"),
        P(),
        P(),
        P(None, "feat"),
        P(None, "feat"),
        P(None, "feat"),
        P("feat", None),
    )
    out_specs = P("seq", "feat")
    return jax.shard_map(
        on_device, mesh=mesh, in_specs=in_specs, out_specs=out_specs, check_vma=False
    )
```

```python
import functools
import math

import jax
import jax.numpy as jnp
from jax import lax
from jax.experimental import pallas as pl
from jax.experimental.pallas import tpu as pltpu
from jax.sharding import PartitionSpec as P

HEADS = 40
KV_HEADS = 8
HEAD_DIM = 128
ITERS = 4

EPS = 1e-06
LAMBDA = 0.03
CHUNKS = 5
HALVES = 4
ROWS = 7
WARM = ITERS
INJ = ITERS + 1
MESH = pl.DeviceIdType.MESH
VMEM = pl.BlockSpec(memory_space=pltpu.VMEM)
ANY = pl.BlockSpec(memory_space=pl.ANY)


def remote(src, dst, send_sem, recv_sem, axis, target):
    return pltpu.make_async_remote_copy(
        src_ref=src, dst_ref=dst, send_sem=send_sem, recv_sem=recv_sem,
        device_id={axis: target}, device_id_type=MESH,
    )


def solve_values(rows, values):
    size = len(values)
    rows = [list(row) for row in rows]
    values = list(values)
    for pivot in range(size):
        for below in range(pivot + 1, size):
            ratio = rows[below][pivot] / rows[pivot][pivot]
            for at in range(pivot, size):
                rows[below][at] = rows[below][at] - ratio * rows[pivot][at]
            values[below] = values[below] - ratio * values[pivot]
    result = [None] * size
    for pivot in reversed(range(size)):
        running = values[pivot]
        for later in range(pivot + 1, size):
            running = running - rows[pivot][later] * result[later]
        result[pivot] = running / rows[pivot][pivot]
    return result


def whole_kernel(n, m, inj_hbm, warm_hbm, gain_in, gain_out, wq_hbm, wk_hbm, wv_hbm, wo_hbm, out,
                 tok, tok_inj, w_kv, w_q, w_o, inj, warm, images, held, proj, base_proj, queries, kv,
                 acc, top, bias, attended, keep, near_out, near, outgoing, far, coef, shares, gram, dots, totals, mixing, sums, norms_out, norms, blend,
                 scale_out, scale_in, mail_out, mail, wide_out, wide,
                 load_sem, feat_s, feat_r, inj_s, inj_r, up_s, up_r, side_s, side_r,
                 near_s, near_r, far_s, far_r, mail_s, mail_r, wide_s, wide_r, norm_s, norm_r):
    me = lax.axis_index("feat")
    side = lax.rem(me, 2)
    mine = lax.div(me, 2)
    partner = me + 1 - 2 * side
    lines = n // 2
    lined = [lax.rem(mine + d, lines) for d in range(lines)]
    before = [lax.rem(mine - d + lines, lines) for d in range(lines)]
    at_seq = lax.axis_index("seq")
    row_side = lax.rem(at_seq, 2)
    level = lax.div(at_seq, 2)
    levels = m // 2
    row_partner = at_seq + 1 - 2 * row_side

    toks, part = inj.shape
    width = n * part
    head_cols = w_q.shape[1]
    kv_cols = w_kv.shape[1] // 2
    kv_local = kv_cols // HEAD_DIM
    heads = head_cols // HEAD_DIM
    group = heads // kv_local
    span = part // CHUNKS
    half = toks // HALVES
    lanes = 128
    scale_all = float(toks * m * width)
    factor = math.log2(math.e) / math.sqrt(HEAD_DIM)
    f32, bf16 = jnp.float32, jnp.bfloat16

    loads = [
        pltpu.make_async_copy(inj_hbm, inj, load_sem.at[0]),
        pltpu.make_async_copy(warm_hbm, warm, load_sem.at[1]),
        pltpu.make_async_copy(wk_hbm, w_kv.at[:, pl.ds(0, kv_cols)], load_sem.at[2]),
        pltpu.make_async_copy(wv_hbm, w_kv.at[:, pl.ds(kv_cols, kv_cols)], load_sem.at[3]),
        pltpu.make_async_copy(wq_hbm, w_q, load_sem.at[4]),
        pltpu.make_async_copy(wo_hbm, w_o, load_sem.at[5]),
    ]
    for load in loads:
        load.start()

    f32_tile = jnp.zeros((8, toks), f32)
    for slot in range(ITERS):
        for owner in range(m):
            norms[slot, owner] = f32_tile

    @pl.when(row_side == 0)
    def _():
        for slot in range(ITERS):
            kv[slot, at_seq + 1] = jnp.zeros(kv.shape[2:], bf16)

    barrier = pltpu.get_barrier_semaphore()
    for d in range(1, n):
        pl.semaphore_signal(barrier, inc=1, device_id={"feat": lax.rem(me + d, n)}, device_id_type=MESH)
    for d in range(1, m):
        pl.semaphore_signal(barrier, inc=1, device_id={"seq": lax.rem(at_seq + d, m)}, device_id_type=MESH)

    def columns(at, size):
        return pl.ds(pl.multiple_of(at * size, size), size)

    def blocks_of(ref_width):
        return ref_width // lanes

    def row_sums(partials):
        rows = [jnp.sum(partial.T, axis=0, keepdims=True) for partial in partials]
        return jnp.concatenate(rows + [jnp.zeros((8 - len(rows), toks), f32)], axis=0)

    def inverse_rms(total):
        return lax.rsqrt(total * (1.0 / width) + EPS)

    def by_token(row):
        return jnp.broadcast_to(row[:1], (lanes, toks)).T

    def everywhere(row):
        return jnp.broadcast_to(row, (8, row.shape[1]))

    zero_tile = jnp.zeros((toks, lanes), f32)

    loads[0].wait()
    loads[1].wait()

    early = (CHUNKS - 1) * span
    count = HALVES + 1

    def gather_copy(buffer, rows, cols, sems, d):
        here = buffer.at[me, rows, cols]
        target = partner if d == 0 else 2 * lined[d] + side
        return remote(here, here, sems[0], sems[1], "feat", target)

    def forward_copy(buffer, rows, cols, sems, d):
        here = buffer.at[2 * before[d] + side, rows, cols]
        return remote(here, here, sems[0], sems[1], "feat", partner)

    def spot(p):
        if isinstance(p, int) and p < 2:
            return pl.ds(0, half), (pl.ds(0, early) if p == 0 else pl.ds(early, part - early))
        return pl.ds(pl.multiple_of((p - 1) * half, half), half), pl.ds(0, part)

    def gather_step(p, d):
        return gather_copy(tok, *spot(p), (feat_s.at[p, d], feat_r.at[p, d]), d)

    def forward_step(p, d):
        at = lines - 1 + d
        return forward_copy(tok, *spot(p), (feat_s.at[p, at], feat_r.at[p, at]), d)

    whole_spot = pl.ds(0, toks), pl.ds(0, part)

    def inj_step(d):
        return gather_copy(tok_inj, *whole_spot, (inj_s.at[d], inj_r.at[d]), d)

    def inj_forward(d):
        at = lines - 1 + d
        return forward_copy(tok_inj, *whole_spot, (inj_s.at[at], inj_r.at[at]), d)

    def start_block(at, totals_now):
        cols = columns(at, lanes)
        gain = gain_in[me, :, cols]
        base = inj[:, cols].astype(f32)
        first = warm[:, cols].astype(f32)
        out[:, cols] = first
        mixed = first + base
        tok[me, :, cols] = (mixed * gain).astype(bf16)
        tok_inj[me, :, cols] = (base * gain).astype(bf16)
        pairs = (first * first, base * base, mixed * mixed)
        return tuple(total + pair for total, pair in zip(totals_now, pairs))

    zero_tile = jnp.zeros((toks, lanes), f32)
    mail_out[1] = row_sums(lax.fori_loop(0, blocks_of(part), start_block, (zero_tile,) * 3))

    def mail_copies(which):
        return [
            remote(mail_out.at[which], mail.at[which, d], mail_s.at[which, d], mail_r.at[which, d],
                   "feat", lax.rem(me + d, n))
            for d in range(1, n)
        ]

    def mail_start(which):
        for copy in mail_copies(which):
            copy.start()

    def mail_total(which):
        total = mail_out[which]
        for d, copy in enumerate(mail_copies(which)):
            copy.wait()
            total = total + mail[which, d + 1]
        return total

    def wide_copies(slot):
        return [
            remote(wide_out, wide.at[slot, d], wide_s.at[slot, d], wide_r.at[slot, d],
                   "seq", lax.rem(at_seq + d, m))
            for d in range(1, m)
        ]

    def wide_total(slot):
        total = wide_out[...]
        for d, copy in enumerate(wide_copies(slot)):
            copy.wait()
            total = total + wide[slot, d + 1]
        return total

    def start_gather(p):
        for d in range(1, lines):
            gather_step(p, d).start()
        gather_step(p, 0).start()

    def relay(p):
        for d in range(1, lines):
            gather_step(p, d).wait_recv()
            forward_step(p, d).start()

    pl.semaphore_wait(barrier, n + m - 2)
    mail_start(1)
    for p in range(count):
        start_gather(p)

    @pl.loop(0, blocks_of(part))
    def _(at):
        cols = columns(at, lanes)
        for j in range(ITERS):
            images[j, :, cols] = zero_tile

    @pl.loop(0, blocks_of(head_cols))
    def _(at):
        cols = columns(at, lanes)
        for j in range(ITERS):
            proj[j, :, cols] = zero_tile

    @pl.loop(0, blocks_of(head_cols + 2 * kv_cols))
    def _(at):
        base_proj[:, columns(at, lanes)] = zero_tile

    small_zero = jnp.zeros((8, lanes), f32)
    for j in range(ITERS):
        coef[j] = jnp.full((8, lanes), 1.0 if j == 0 else 0.0, f32)
        shares[j] = jnp.full((8, lanes), 1.0 if j == 0 else 0.0, f32)
    for j in range(ITERS * ITERS):
        gram[j] = small_zero
    for j in range((WARM + 1) * (WARM + 1)):
        totals[j] = small_zero
    for j in range(ITERS * (WARM + 1)):
        mixing[j] = small_zero
    for j in range((INJ + 1) * (INJ + 1)):
        dots[j] = jnp.zeros((8, toks), f32)
    scale_out[...] = jnp.ones((toks, lanes), f32)

    key_at = lax.broadcasted_iota(jnp.int32, (toks, 2 * toks), 1)
    query_at = lax.broadcasted_iota(jnp.int32, (toks, 2 * toks), 0) + row_side * toks
    bias[0] = jnp.where(key_at <= query_at, 0.0, -1e30).astype(f32)
    bias[1] = jnp.zeros((toks, 2 * toks), f32)

    def dot_at(i, j):
        return dots[(INJ + 1) * i + j]

    def total_at(i, j):
        return totals[(WARM + 1) * i + j]

    def settle_first(k, slot):
        total = mail_total(0)
        rate = inverse_rms(total[:1])
        scale_out[...] = by_token(rate)
        for at, j in enumerate(list(range(ITERS - 1)) + [WARM, INJ]):
            value = everywhere(total[at + 1 : at + 2] * rate)
            dots[(INJ + 1) * k + j] = value
            dots[(INJ + 1) * j + k] = value
        dots[(INJ + 2) * k] = everywhere(total[ROWS - 1 : ROWS] * rate * rate)
        for j in range(WARM + 1):
            before_now = jnp.where(k == 0, 1.0 if j == WARM else 0.0, coef[j] if j < WARM else 0.0)
            mixing[(WARM + 1) * k + j] = jnp.where(k == j, 1.0, 0.0) - before_now * jnp.ones((8, lanes), f32)

        @pl.when(k > 0)
        def _():
            rows = [dots[(INJ + 1) * k + j][:1] for j in range(WARM + 1)]
            rows = rows + [dot_at(0, 0)[:1], dot_at(0, WARM)[:1], dot_at(WARM, WARM)[:1]]
            wide_out[...] = jnp.concatenate(rows, axis=0)
            for copy in wide_copies(slot):
                copy.start()

    def settle_last(k, slot):
        @pl.when(k > 0)
        def _():
            total = jnp.broadcast_to(jnp.sum(wide_total(slot), axis=1, keepdims=True), (8, lanes))
            values = [jnp.broadcast_to(total[j : j + 1], (8, lanes)) for j in range(8)]
            for j in range(WARM + 1):
                totals[(WARM + 1) * k + j] = values[j]
                totals[(WARM + 1) * j + k] = values[j]
            totals[0] = values[WARM + 1]
            totals[WARM] = values[WARM + 2]
            totals[(WARM + 1) * WARM] = values[WARM + 2]
            totals[(WARM + 1) * WARM + WARM] = values[WARM + 3]

            def product(i, j):
                run = small_zero
                for a in range(WARM + 1):
                    inner = small_zero
                    for b in range(WARM + 1):
                        inner = inner + total_at(a, b) * mixing[(WARM + 1) * j + b]
                    run = run + mixing[(WARM + 1) * i + a] * inner
                return run

            gram[0] = product(0, 0)
            for j in range(ITERS):
                value = product(j, k)
                gram[ITERS * k + j] = value
                gram[ITERS * j + k] = value
            system = []
            for i in range(ITERS):
                row = []
                for j in range(ITERS):
                    fixed = LAMBDA if i == j else 0.0
                    there = gram[ITERS * i + j] / scale_all + fixed
                    row.append(jnp.where(max(i, j) <= k, there, 1.0 if i == j else 0.0))
                system.append(row)
            goals = [jnp.where(i <= k, jnp.ones((8, lanes), f32), 0.0) for i in range(ITERS)]
            unscaled = solve_values(system, goals)
            whole = unscaled[0]
            for value in unscaled[1:]:
                whole = whole + value
            for j in range(ITERS):
                coef[j] = unscaled[j] / whole

        parts_now = [jnp.broadcast_to(coef[j][:, :1], (8, toks)) for j in range(ITERS)]
        square = dot_at(INJ, INJ)
        for i in range(ITERS):
            inner = 2.0 * dot_at(i, INJ)
            for j in range(ITERS):
                inner = inner + parts_now[j] * dot_at(i, j)
            square = square + parts_now[i] * inner
        return inverse_rms(jnp.maximum(square, 0.0))

    def remix(k):
        @pl.loop(0, blocks_of(part))
        def _(at):
            cols = columns(at, lanes)
            images[k, :, cols] = held[:, cols] * scale_out[...] * gain_out[me, :, cols]
            current = coef[0][:1] * images[0, :, cols]
            for j in range(1, ITERS):
                current = current + coef[j][:1] * images[j, :, cols]
            out[:, cols] = current

    def kv_copy(slot, c, owner, sems, target):
        here = kv.at[slot, owner, pl.ds(c * half, half)]
        return remote(here, here, sems[0], sems[1], "seq", target)

    def up_step(it, c, k, owner, target):
        return kv_copy(it, c, owner, (up_s.at[c, k], up_r.at[it, c, k]), target)

    def side_step(it, c, k, owner):
        return kv_copy(it, c, owner, (side_s.at[c, k], side_r.at[it, c, k]), row_partner)

    def norm_step(it, d, owner, target):
        return remote(norms_out, norms.at[it, owner], norm_s.at[d], norm_r.at[it, d], "seq", target)

    def share_norms(it, row):
        norms_out[...] = everywhere(row)
        norms[it, at_seq] = everywhere(row)
        scale_in[...] = by_token(row)
        for d in range(m - 1, 0, -1):
            @pl.when(at_seq + d < m)
            def _():
                norm_step(it, d, at_seq, at_seq + d).start()

    def project(buffer, rows, weights, cols):
        tokens = jnp.concatenate([buffer[f, rows, :] for f in range(n)], axis=1)
        return jnp.dot(tokens, weights[:, cols], preferred_element_type=f32)

    def wide_scale(tile, size):
        return jnp.concatenate([tile] * (size // lanes), axis=1)

    q_tile = span
    kv_tile = min(256, 2 * kv_cols)

    def attend(it, k):
        which = min(k, 1)
        pairs = []
        for o in range(2):
            owner = 2 * (level - k) + o
            first = jnp.minimum(it, 1)
            blend[o] = shares[first][:1, :1] * kv[first, owner].astype(f32)
            for j in range(2, ITERS):
                @pl.when(it >= j)
                def _():
                    blend[o] += shares[j][:1, :1] * kv[j, owner].astype(f32)

            rate = by_token(norms[it, owner])
            pairs.append((blend[o] * wide_scale(rate, 2 * kv_cols)).astype(bf16))
        pair = jnp.concatenate(pairs, axis=0)
        for e in range(kv_local):
            keys = pair[:, e * HEAD_DIM : (e + 1) * HEAD_DIM]
            values = pair[:, kv_cols + e * HEAD_DIM : kv_cols + (e + 1) * HEAD_DIM]
            values = jnp.concatenate([values, jnp.ones((2 * toks, HEAD_DIM), bf16)], axis=1)
            asked = queries[e * group : (e + 1) * group].reshape(group * toks, HEAD_DIM)
            scores = lax.dot_general(asked, keys, (((1,), (1,)), ((), ())), preferred_element_type=f32)
            scores = (scores.reshape(group, toks, 2 * toks) + bias[which][None]).reshape(group * toks, 2 * toks)
            old = top[e]
            new = jnp.maximum(old, jnp.max(scores, axis=1, keepdims=True))
            top[e] = new
            both = jnp.concatenate([new] * (2 * toks // lanes), axis=1)
            weights = jnp.exp2((scores - both) * factor)
            fade = jnp.exp2((old - new) * factor)
            acc[e] = acc[e] * jnp.concatenate([fade, fade], axis=1) + jnp.dot(
                weights.astype(bf16), values, preferred_element_type=f32
            )

    def near_step(c, d):
        return remote(
            near_out.at[d, :, columns(c, span)], near.at[d, :, columns(c, span)],
            near_s.at[c, d], near_r.at[c, d], "feat", partner,
        )

    def far_step(c, d):
        return remote(
            outgoing.at[d, :, columns(c, span)], far.at[d, :, columns(c, span)],
            far_s.at[c, d], far_r.at[c, d], "feat", 2 * lined[d] + side,
        )

    def out_dot(target, c):
        cols = pl.ds(pl.multiple_of(target * part + c * span, span), span)
        return jnp.dot(attended[...], w_o[:, cols], preferred_element_type=f32)

    def pass_on(c):
        cols = columns(c, span)
        for d in range(1, lines):
            near_step(c, d).wait_recv()
            outgoing[d, :, cols] = (keep[d, :, cols] + near[d, :, cols].astype(f32)).astype(bf16)
            far_step(c, d).start()

    def own_dots(c):
        cols = columns(c, span)
        near_out[0, :, cols] = out_dot(2 * mine + 1 - side, c).astype(bf16)
        near_step(c, 0).start()
        keep[0, :, cols] = out_dot(me, c)

    def arrive(it, c, k):
        @pl.when(k <= level)
        def _():
            owner = at_seq - 2 * k
            up_step(it, c, k - 1, owner, owner).wait_recv()

            @pl.when(level + 1 < levels)
            def _():
                up_step(it, c, k, owner, at_seq + 2).start()

            side_step(it, c, k, owner).start()

    def all_rows():
        return pl.ds(0, toks)

    def collect(p):
        gather_step(p, 0).wait()
        for d in range(1, lines):
            forward_step(p, d).wait()
            gather_step(p, d).wait_send()

    def send_keys(it, c):
        rows = pl.ds(c * half, half) if isinstance(c, int) else pl.ds(pl.multiple_of(c * half, half), half)
        for at in range(2 * kv_cols // kv_tile):
            cols = pl.ds(at * kv_tile, kv_tile)
            there = project(tok, rows, w_kv, cols) * wide_scale(scale_out[rows, :], kv_tile)
            kv[it, at_seq, rows, cols] = (there + base_proj[rows, cols]).astype(bf16)

        @pl.when(row_side == 0)
        def _():
            side_step(it, c, 0, at_seq).start()

        @pl.when(level + 1 < levels)
        def _():
            up_step(it, c, 0, at_seq, at_seq + 2).start()

    def ask(it, at):
        cols = columns(at, q_tile)
        there = project(tok, all_rows(), w_q, cols) * wide_scale(scale_out[...], q_tile)
        proj[it, :, cols] = there + base_proj[:, pl.ds(pl.multiple_of(2 * kv_cols + at * q_tile, q_tile), q_tile)]
        total = shares[0][:1, :1] * proj[0, :, cols]
        for j in range(1, ITERS):
            total = total + shares[j][:1, :1] * proj[j, :, cols]
        asked = (total * wide_scale(scale_in[...], q_tile)).astype(bf16)
        for h in range(q_tile // HEAD_DIM):
            queries[at * (q_tile // HEAD_DIM) + h] = asked[:, h * HEAD_DIM : (h + 1) * HEAD_DIM]

    def project_base():
        for d in range(1, lines):
            inj_forward(d).wait()
        inj_step(0).wait()
        for d in range(1, lines):
            inj_step(d).wait_send()

        @pl.loop(0, 2 * kv_cols // kv_tile)
        def _(at):
            cols = columns(at, kv_tile)
            base_proj[:, cols] = project(tok_inj, all_rows(), w_kv, cols)

        @pl.loop(0, head_cols // q_tile)
        def _(at):
            put = pl.ds(pl.multiple_of(2 * kv_cols + at * q_tile, q_tile), q_tile)
            base_proj[:, put] = project(tok_inj, all_rows(), w_q, columns(at, q_tile))

    hops = sorted(((c, k) for c in range(HALVES) for k in range(1, levels)), key=lambda one: one[0] + 3 * one[1])

    def evaluate(it):
        k = jnp.maximum(it - 1, 0)
        slot = lax.rem(it, 2)
        waiting = list(hops)
        met = []

        def forward(count):
            for c, j in waiting[:count]:
                arrive(it, c, j)
                waiting.remove((c, j))
                if all(other[1] != j for other in waiting):
                    met.append(j - 1)

        relay(0)
        relay(1)

        @pl.when(it > 0)
        def _():
            settle_first(k, slot)

        @pl.when(it == 0)
        def _():
            loads[2].wait()
            loads[3].wait()

        collect(0)
        collect(1)
        send_keys(it, 0)
        relay(2)

        @pl.loop(1, HALVES)
        def _(c):
            collect(c + 1)

            @pl.when(c + 1 < HALVES)
            def _():
                relay(c + 2)

            send_keys(it, c)

            @pl.when(c == HALVES - 2)
            def _():
                for one in waiting[:1]:
                    arrive(it, *one)

        del waiting[:1]
        forward(2)

        @pl.when(it > 0)
        def _():
            share_norms(it, settle_last(k, slot)[:1])
            shares[0] = jnp.zeros((8, lanes), f32)
            for j in range(1, ITERS):
                shares[j] = coef[j - 1]

        @pl.when(it == 0)
        def _():
            total = mail_total(1)
            dots[(INJ + 1) * WARM + WARM] = everywhere(total[:1])
            dots[(INJ + 1) * INJ + INJ] = everywhere(total[1:2])
            share_norms(it, inverse_rms(total[2:3]))
            loads[4].wait()
            for d in range(lines):
                inj_step(d).start()

        q_tiles = head_cols // q_tile
        early_hops = waiting[:q_tiles]

        @pl.loop(0, q_tiles)
        def _(at):
            ask(it, at)
            for index, one in enumerate(early_hops):
                @pl.when(at == index)
                def _():
                    arrive(it, *one)

        met.extend(sorted({j - 1 for c, j in early_hops if all(other[1] != j for other in waiting[q_tiles:])}))
        del waiting[:q_tiles]

        @pl.when(it > 0)
        def _():
            remix(k)

        for e in range(kv_local):
            top[e] = jnp.full(top.shape[1:], -1e30, f32)
            acc[e] = jnp.zeros(acc.shape[1:], f32)

        def meet(k):
            @pl.when(k <= level)
            def _():
                @pl.when(k + row_side > 0)
                def _():
                    for c in range(HALVES):
                        side_step(it, c, k, row_partner - 2 * k).wait_recv()

                for o in range(2):
                    d = 2 * k - o + row_side

                    @pl.when((d > 0) & (at_seq - d >= 0))
                    def _():
                        norm_step(it, d, at_seq, at_seq - d).wait_recv()

                attend(it, k)

        while waiting:
            for k in met:
                meet(k)
            met.clear()
            forward(1)
        for k in met + [levels - 1]:
            meet(k)

        for e in range(kv_local):
            for g in range(group):
                rows = slice(g * toks, (g + 1) * toks)
                at = (e * group + g) * HEAD_DIM
                attended[:, at : at + HEAD_DIM] = (
                    acc[e, rows, :HEAD_DIM] / acc[e, rows, HEAD_DIM:]
                ).astype(bf16)

        @pl.when(it == 0)
        def _():
            loads[5].wait()
            for d in range(1, lines):
                inj_step(d).wait_recv()
                inj_forward(d).start()

        @pl.loop(0, CHUNKS)
        def _(c):
            cols = columns(c, span)
            for d in range(1, lines):
                near_out[d, :, cols] = out_dot(2 * lined[d] + 1 - side, c).astype(bf16)
                near_step(c, d).start()
                keep[d, :, cols] = out_dot(2 * lined[d] + side, c)

            @pl.when(c > 0)
            def _():
                pass_on(c - 1)

        own_dots(0)
        pass_on(CHUNKS - 1)

        @pl.loop(1, CHUNKS)
        def _(c):
            own_dots(c)

        @pl.when(it == 0)
        def _():
            project_base()

        for at in range(ROWS):
            sums[at] = zero_tile

        @pl.loop(0, CHUNKS)
        def _(c):
            near_step(c, 0).wait()
            for d in range(1, lines):
                near_step(c, d).wait_send()
                far_step(c, d).wait()
            for at in range(span // lanes):
                cols = pl.ds(pl.multiple_of(c * span + at * lanes, lanes), lanes)
                update = keep[0, :, cols] + near[0, :, cols].astype(f32)
                for d in range(1, lines):
                    update = update + far[d, :, cols].astype(f32)
                base = inj[:, cols].astype(f32)
                summed = out[:, cols] + base + update
                held[:, cols] = summed
                scaled = summed * gain_out[me, :, cols]
                tok[me, :, cols] = (scaled * gain_in[me, :, cols]).astype(bf16)
                others = [images[j, :, cols] for j in range(ITERS - 1)]
                others = others + [warm[:, cols].astype(f32), base, scaled]
                sums[0] += summed * summed
                for row, other in enumerate(others):
                    sums[row + 1] += scaled * other

            @pl.when((it + 1 < ITERS) & (c == CHUNKS - 2))
            def _():
                start_gather(0)

        mail_out[0] = row_sums([sums[at] for at in range(ROWS)])
        mail_start(0)

        @pl.when(it + 1 < ITERS)
        def _():
            for p in range(1, count):
                start_gather(p)

        for c in range(HALVES):
            @pl.when(row_side == 0)
            def _():
                side_step(it, c, 0, at_seq).wait_send()

            @pl.when(level + 1 < levels)
            def _():
                up_step(it, c, 0, at_seq, at_seq + 2).wait_send()

        @pl.loop(1, level + 1)
        def _(k):
            for c in range(HALVES):
                side_step(it, c, k, at_seq - 2 * k).wait_send()

                @pl.when(level + 1 < levels)
                def _():
                    up_step(it, c, k, at_seq - 2 * k, at_seq + 2).wait_send()

        for d in range(1, m):
            @pl.when(at_seq + d < m)
            def _():
                norm_step(it, d, at_seq, at_seq + d).wait_send()

    @pl.loop(0, ITERS)
    def _(it):
        evaluate(it)

    settle_first(ITERS - 1, lax.rem(ITERS, 2))
    settle_last(ITERS - 1, lax.rem(ITERS, 2))
    remix(ITERS - 1)


def on_device(injection, warm_start, gain_in, gain_out, w_query, w_key, w_value, w_out):
    n, m = lax.axis_size("feat"), lax.axis_size("seq")
    toks, part = injection.shape
    head_cols, kv_cols = w_query.shape[1], w_key.shape[1]
    kv_local = kv_cols // HEAD_DIM
    group = HEADS // KV_HEADS
    lines = n // 2
    f32, bf16 = jnp.float32, jnp.bfloat16
    vmem, dma = pltpu.VMEM, pltpu.SemaphoreType.DMA
    lanes = 128
    scratch = [
        vmem((n, toks, part), bf16), vmem((n, toks, part), bf16),
        vmem((w_key.shape[0], 2 * kv_cols), bf16), vmem(w_query.shape, bf16), vmem(w_out.shape, bf16),
        vmem((toks, part), bf16), vmem((toks, part), bf16),
        vmem((ITERS, toks, part), f32), vmem((toks, part), f32),
        vmem((ITERS, toks, head_cols), f32), vmem((toks, head_cols + 2 * kv_cols), f32),
        vmem((head_cols // HEAD_DIM, toks, HEAD_DIM), bf16),
        vmem((ITERS, m, toks, 2 * kv_cols), bf16),
        vmem((kv_local, group * toks, 2 * HEAD_DIM), f32), vmem((kv_local, group * toks, lanes), f32),
        vmem((2, toks, 2 * toks), f32), vmem((toks, head_cols), bf16),
        vmem((lines, toks, part), f32),
        vmem((lines, toks, part), bf16), vmem((lines, toks, part), bf16),
        vmem((lines, toks, part), bf16), vmem((lines, toks, part), bf16),
        vmem((ITERS, 8, lanes), f32), vmem((ITERS, 8, lanes), f32), vmem((ITERS * ITERS, 8, lanes), f32),
        vmem(((INJ + 1) * (INJ + 1), 8, toks), f32), vmem(((WARM + 1) * (WARM + 1), 8, lanes), f32),
        vmem((ITERS * (WARM + 1), 8, lanes), f32), vmem((ROWS, toks, lanes), f32),
        vmem((8, toks), f32), vmem((ITERS, m, 8, toks), f32), vmem((2, toks, 2 * kv_cols), f32),
        vmem((toks, lanes), f32), vmem((toks, lanes), f32),
        vmem((3, 8, toks), f32), vmem((3, n, 8, toks), f32),
        vmem((8, lanes), f32), vmem((2, m, 8, lanes), f32),
        dma((6,)), dma((HALVES + 1, n)), dma((HALVES + 1, n)), dma((n,)), dma((n,)),
        dma((HALVES, m // 2)), dma((ITERS, HALVES, m // 2)), dma((HALVES, m // 2)), dma((ITERS, HALVES, m // 2)),
        dma((CHUNKS, lines)), dma((CHUNKS, lines)), dma((CHUNKS, lines)), dma((CHUNKS, lines)),
        dma((3, n)), dma((3, n)), dma((2, m)), dma((2, m)), dma((m,)), dma((ITERS, m)),
    ]
    return pl.pallas_call(
        functools.partial(whole_kernel, n, m),
        out_shape=jax.ShapeDtypeStruct((toks, part), f32),
        in_specs=[ANY, ANY, VMEM, VMEM, ANY, ANY, ANY, ANY],
        out_specs=VMEM,
        scratch_shapes=scratch,
        compiler_params=pltpu.CompilerParams(
            collective_id=0, has_side_effects=True, vmem_limit_bytes=63 * 1024 * 1024
        ),
    )(
        injection, warm_start, gain_in.reshape(n, 1, part), gain_out.reshape(n, 1, part),
        w_query, w_key, w_value, w_out,
    )


def solution(mesh):
    in_specs = (
        P("seq", "feat"),
        P("seq", "feat"),
        P(),
        P(),
        P(None, "feat"),
        P(None, "feat"),
        P(None, "feat"),
        P("feat", None),
    )
    out_specs = P("seq", "feat")
    return jax.shard_map(
        on_device, mesh=mesh, in_specs=in_specs, out_specs=out_specs, check_vma=False
    )
```

```python
import functools
import math

import jax
import jax.numpy as jnp
from jax import lax
from jax.experimental import pallas as pl
from jax.experimental.pallas import tpu as pltpu
from jax.sharding import PartitionSpec as P

HEADS = 40
KV_HEADS = 8
HEAD_DIM = 128
ITERS = 4

EPS = 1e-06
LAMBDA = 0.03
CHUNKS = 5
HALVES = 4
ROWS = 7
WARM = ITERS
INJ = ITERS + 1
MESH = pl.DeviceIdType.MESH
VMEM = pl.BlockSpec(memory_space=pltpu.VMEM)
ANY = pl.BlockSpec(memory_space=pl.ANY)


def remote(src, dst, send_sem, recv_sem, axis, target):
    return pltpu.make_async_remote_copy(
        src_ref=src, dst_ref=dst, send_sem=send_sem, recv_sem=recv_sem,
        device_id={axis: target}, device_id_type=MESH,
    )


def solve_values(rows, values):
    size = len(values)
    rows = [list(row) for row in rows]
    values = list(values)
    for pivot in range(size):
        for below in range(pivot + 1, size):
            ratio = rows[below][pivot] / rows[pivot][pivot]
            for at in range(pivot, size):
                rows[below][at] = rows[below][at] - ratio * rows[pivot][at]
            values[below] = values[below] - ratio * values[pivot]
    result = [None] * size
    for pivot in reversed(range(size)):
        running = values[pivot]
        for later in range(pivot + 1, size):
            running = running - rows[pivot][later] * result[later]
        result[pivot] = running / rows[pivot][pivot]
    return result


def whole_kernel(n, m, inj_hbm, warm_hbm, gain_in, gain_out, wq_hbm, wk_hbm, wv_hbm, wo_hbm, out,
                 tok, tok_inj, w_kv, w_q, w_o, inj, warm, images, held, proj, base_proj, queries, kv,
                 acc, top, bias, attended, keep, near_out, near, outgoing, far, coef, shares, gram, dots, totals, mixing, sums, norms_out, norms,
                 scale_out, scale_in, mail_out, mail, wide_out, wide,
                 load_sem, feat_s, feat_r, inj_s, inj_r, up_s, up_r, side_s, side_r,
                 near_s, near_r, far_s, far_r, mail_s, mail_r, wide_s, wide_r, norm_s, norm_r):
    me = lax.axis_index("feat")
    side = lax.rem(me, 2)
    mine = lax.div(me, 2)
    partner = me + 1 - 2 * side
    lines = n // 2
    lined = [lax.rem(mine + d, lines) for d in range(lines)]
    before = [lax.rem(mine - d + lines, lines) for d in range(lines)]
    at_seq = lax.axis_index("seq")
    row_side = lax.rem(at_seq, 2)
    level = lax.div(at_seq, 2)
    levels = m // 2
    row_partner = at_seq + 1 - 2 * row_side

    toks, part = inj.shape
    width = n * part
    head_cols = w_q.shape[1]
    kv_cols = w_kv.shape[1] // 2
    kv_local = kv_cols // HEAD_DIM
    heads = head_cols // HEAD_DIM
    group = heads // kv_local
    span = part // CHUNKS
    half = toks // HALVES
    lanes = 128
    scale_all = float(toks * m * width)
    factor = math.log2(math.e) / math.sqrt(HEAD_DIM)
    f32, bf16 = jnp.float32, jnp.bfloat16

    loads = [
        pltpu.make_async_copy(inj_hbm, inj, load_sem.at[0]),
        pltpu.make_async_copy(warm_hbm, warm, load_sem.at[1]),
        pltpu.make_async_copy(wk_hbm, w_kv.at[:, pl.ds(0, kv_cols)], load_sem.at[2]),
        pltpu.make_async_copy(wv_hbm, w_kv.at[:, pl.ds(kv_cols, kv_cols)], load_sem.at[3]),
        pltpu.make_async_copy(wq_hbm, w_q, load_sem.at[4]),
        pltpu.make_async_copy(wo_hbm, w_o, load_sem.at[5]),
    ]
    for load in loads:
        load.start()

    f32_tile = jnp.zeros((8, toks), f32)
    for slot in range(ITERS):
        for owner in range(m):
            norms[slot, owner] = f32_tile

    @pl.when(row_side == 0)
    def _():
        for slot in range(ITERS):
            kv[slot, at_seq + 1] = jnp.zeros(kv.shape[2:], bf16)

    barrier = pltpu.get_barrier_semaphore()
    for d in range(1, n):
        pl.semaphore_signal(barrier, inc=1, device_id={"feat": lax.rem(me + d, n)}, device_id_type=MESH)
    for d in range(1, m):
        pl.semaphore_signal(barrier, inc=1, device_id={"seq": lax.rem(at_seq + d, m)}, device_id_type=MESH)

    def columns(at, size):
        return pl.ds(pl.multiple_of(at * size, size), size)

    def blocks_of(ref_width):
        return ref_width // lanes

    def row_sums(partials):
        rows = [jnp.sum(partial.T, axis=0, keepdims=True) for partial in partials]
        return jnp.concatenate(rows + [jnp.zeros((8 - len(rows), toks), f32)], axis=0)

    def inverse_rms(total):
        return lax.rsqrt(total * (1.0 / width) + EPS)

    def by_token(row):
        return jnp.broadcast_to(row[:1], (lanes, toks)).T

    def everywhere(row):
        return jnp.broadcast_to(row, (8, row.shape[1]))

    zero_tile = jnp.zeros((toks, lanes), f32)

    loads[0].wait()
    loads[1].wait()

    early = (CHUNKS - 1) * span
    count = HALVES + 1

    def gather_copy(buffer, rows, cols, sems, d):
        here = buffer.at[me, rows, cols]
        target = partner if d == 0 else 2 * lined[d] + side
        return remote(here, here, sems[0], sems[1], "feat", target)

    def forward_copy(buffer, rows, cols, sems, d):
        here = buffer.at[2 * before[d] + side, rows, cols]
        return remote(here, here, sems[0], sems[1], "feat", partner)

    def spot(p):
        if isinstance(p, int) and p < 2:
            return pl.ds(0, half), (pl.ds(0, early) if p == 0 else pl.ds(early, part - early))
        return pl.ds(pl.multiple_of((p - 1) * half, half), half), pl.ds(0, part)

    def gather_step(p, d):
        return gather_copy(tok, *spot(p), (feat_s.at[p, d], feat_r.at[p, d]), d)

    def forward_step(p, d):
        at = lines - 1 + d
        return forward_copy(tok, *spot(p), (feat_s.at[p, at], feat_r.at[p, at]), d)

    whole_spot = pl.ds(0, toks), pl.ds(0, part)

    def inj_step(d):
        return gather_copy(tok_inj, *whole_spot, (inj_s.at[d], inj_r.at[d]), d)

    def inj_forward(d):
        at = lines - 1 + d
        return forward_copy(tok_inj, *whole_spot, (inj_s.at[at], inj_r.at[at]), d)

    def start_block(at, totals_now):
        cols = columns(at, lanes)
        gain = gain_in[me, :, cols]
        base = inj[:, cols].astype(f32)
        first = warm[:, cols].astype(f32)
        out[:, cols] = first
        mixed = first + base
        tok[me, :, cols] = (mixed * gain).astype(bf16)
        tok_inj[me, :, cols] = (base * gain).astype(bf16)
        pairs = (first * first, base * base, mixed * mixed)
        return tuple(total + pair for total, pair in zip(totals_now, pairs))

    zero_tile = jnp.zeros((toks, lanes), f32)
    mail_out[1] = row_sums(lax.fori_loop(0, blocks_of(part), start_block, (zero_tile,) * 3))

    def mail_copies(which):
        return [
            remote(mail_out.at[which], mail.at[which, d], mail_s.at[which, d], mail_r.at[which, d],
                   "feat", lax.rem(me + d, n))
            for d in range(1, n)
        ]

    def mail_start(which):
        for copy in mail_copies(which):
            copy.start()

    def mail_total(which):
        total = mail_out[which]
        for d, copy in enumerate(mail_copies(which)):
            copy.wait()
            total = total + mail[which, d + 1]
        return total

    def wide_copies(slot):
        return [
            remote(wide_out, wide.at[slot, d], wide_s.at[slot, d], wide_r.at[slot, d],
                   "seq", lax.rem(at_seq + d, m))
            for d in range(1, m)
        ]

    def wide_total(slot):
        total = wide_out[...]
        for d, copy in enumerate(wide_copies(slot)):
            copy.wait()
            total = total + wide[slot, d + 1]
        return total

    def start_gather(p):
        for d in range(1, lines):
            gather_step(p, d).start()
        gather_step(p, 0).start()

    def relay(p):
        for d in range(1, lines):
            gather_step(p, d).wait_recv()
            forward_step(p, d).start()

    pl.semaphore_wait(barrier, n + m - 2)
    mail_start(1)
    for p in range(count):
        start_gather(p)

    @pl.loop(0, blocks_of(part))
    def _(at):
        cols = columns(at, lanes)
        for j in range(ITERS):
            images[j, :, cols] = zero_tile

    @pl.loop(0, blocks_of(head_cols))
    def _(at):
        cols = columns(at, lanes)
        for j in range(ITERS):
            proj[j, :, cols] = zero_tile

    @pl.loop(0, blocks_of(head_cols + 2 * kv_cols))
    def _(at):
        base_proj[:, columns(at, lanes)] = zero_tile

    small_zero = jnp.zeros((8, lanes), f32)
    for j in range(ITERS):
        coef[j] = jnp.full((8, lanes), 1.0 if j == 0 else 0.0, f32)
        shares[j] = jnp.full((8, lanes), 1.0 if j == 0 else 0.0, f32)
    for j in range(ITERS * ITERS):
        gram[j] = small_zero
    for j in range((WARM + 1) * (WARM + 1)):
        totals[j] = small_zero
    for j in range(ITERS * (WARM + 1)):
        mixing[j] = small_zero
    for j in range((INJ + 1) * (INJ + 1)):
        dots[j] = jnp.zeros((8, toks), f32)
    scale_out[...] = jnp.ones((toks, lanes), f32)

    key_at = lax.broadcasted_iota(jnp.int32, (toks, 2 * toks), 1)
    query_at = lax.broadcasted_iota(jnp.int32, (toks, 2 * toks), 0) + row_side * toks
    bias[0] = jnp.where(key_at <= query_at, 0.0, -1e30).astype(f32)
    bias[1] = jnp.zeros((toks, 2 * toks), f32)

    def dot_at(i, j):
        return dots[(INJ + 1) * i + j]

    def total_at(i, j):
        return totals[(WARM + 1) * i + j]

    def settle_first(k, slot):
        total = mail_total(0)
        rate = inverse_rms(total[:1])
        scale_out[...] = by_token(rate)
        for at, j in enumerate(list(range(ITERS - 1)) + [WARM, INJ]):
            value = everywhere(total[at + 1 : at + 2] * rate)
            dots[(INJ + 1) * k + j] = value
            dots[(INJ + 1) * j + k] = value
        dots[(INJ + 2) * k] = everywhere(total[ROWS - 1 : ROWS] * rate * rate)
        for j in range(WARM + 1):
            before_now = jnp.where(k == 0, 1.0 if j == WARM else 0.0, coef[j] if j < WARM else 0.0)
            mixing[(WARM + 1) * k + j] = jnp.where(k == j, 1.0, 0.0) - before_now * jnp.ones((8, lanes), f32)

        @pl.when(k > 0)
        def _():
            rows = [dots[(INJ + 1) * k + j][:1] for j in range(WARM + 1)]
            rows = rows + [dot_at(0, 0)[:1], dot_at(0, WARM)[:1], dot_at(WARM, WARM)[:1]]
            wide_out[...] = jnp.concatenate(rows, axis=0)
            for copy in wide_copies(slot):
                copy.start()

    def settle_last(k, slot):
        @pl.when(k > 0)
        def _():
            total = jnp.broadcast_to(jnp.sum(wide_total(slot), axis=1, keepdims=True), (8, lanes))
            values = [jnp.broadcast_to(total[j : j + 1], (8, lanes)) for j in range(8)]
            for j in range(WARM + 1):
                totals[(WARM + 1) * k + j] = values[j]
                totals[(WARM + 1) * j + k] = values[j]
            totals[0] = values[WARM + 1]
            totals[WARM] = values[WARM + 2]
            totals[(WARM + 1) * WARM] = values[WARM + 2]
            totals[(WARM + 1) * WARM + WARM] = values[WARM + 3]

            def product(i, j):
                run = small_zero
                for a in range(WARM + 1):
                    inner = small_zero
                    for b in range(WARM + 1):
                        inner = inner + total_at(a, b) * mixing[(WARM + 1) * j + b]
                    run = run + mixing[(WARM + 1) * i + a] * inner
                return run

            gram[0] = product(0, 0)
            for j in range(ITERS):
                value = product(j, k)
                gram[ITERS * k + j] = value
                gram[ITERS * j + k] = value
            system = []
            for i in range(ITERS):
                row = []
                for j in range(ITERS):
                    fixed = LAMBDA if i == j else 0.0
                    there = gram[ITERS * i + j] / scale_all + fixed
                    row.append(jnp.where(max(i, j) <= k, there, 1.0 if i == j else 0.0))
                system.append(row)
            goals = [jnp.where(i <= k, jnp.ones((8, lanes), f32), 0.0) for i in range(ITERS)]
            unscaled = solve_values(system, goals)
            whole = unscaled[0]
            for value in unscaled[1:]:
                whole = whole + value
            for j in range(ITERS):
                coef[j] = unscaled[j] / whole

        parts_now = [jnp.broadcast_to(coef[j][:, :1], (8, toks)) for j in range(ITERS)]
        square = dot_at(INJ, INJ)
        for i in range(ITERS):
            inner = 2.0 * dot_at(i, INJ)
            for j in range(ITERS):
                inner = inner + parts_now[j] * dot_at(i, j)
            square = square + parts_now[i] * inner
        return inverse_rms(jnp.maximum(square, 0.0))

    def remix(k):
        @pl.loop(0, blocks_of(part))
        def _(at):
            cols = columns(at, lanes)
            images[k, :, cols] = held[:, cols] * scale_out[...] * gain_out[me, :, cols]
            current = coef[0][:1] * images[0, :, cols]
            for j in range(1, ITERS):
                current = current + coef[j][:1] * images[j, :, cols]
            out[:, cols] = current

    def kv_copy(slot, c, owner, sems, target):
        here = kv.at[slot, owner, pl.ds(c * half, half)]
        return remote(here, here, sems[0], sems[1], "seq", target)

    def up_step(it, c, k, owner, target):
        return kv_copy(it, c, owner, (up_s.at[c, k], up_r.at[it, c, k]), target)

    def side_step(it, c, k, owner):
        return kv_copy(it, c, owner, (side_s.at[c, k], side_r.at[it, c, k]), row_partner)

    def norm_step(it, d, owner, target):
        return remote(norms_out, norms.at[it, owner], norm_s.at[d], norm_r.at[it, d], "seq", target)

    def share_norms(it, row):
        norms_out[...] = everywhere(row)
        norms[it, at_seq] = everywhere(row)
        scale_in[...] = by_token(row)
        for d in range(m - 1, 0, -1):
            @pl.when(at_seq + d < m)
            def _():
                norm_step(it, d, at_seq, at_seq + d).start()

    def project(buffer, rows, weights, cols):
        tokens = jnp.concatenate([buffer[f, rows, :] for f in range(n)], axis=1)
        return jnp.dot(tokens, weights[:, cols], preferred_element_type=f32)

    def wide_scale(tile, size):
        return jnp.concatenate([tile] * (size // lanes), axis=1)

    q_tile = span
    kv_tile = min(256, 2 * kv_cols)

    def attend(it, k):
        which = min(k, 1)
        pairs = []
        for o in range(2):
            owner = 2 * (level - k) + o
            first = jnp.minimum(it, 1)
            mixed = shares[first][:1, :1] * kv[first, owner].astype(f32)
            for j in range(2, ITERS):
                mixed = mixed + shares[j][:1, :1] * kv[jnp.minimum(j, it), owner].astype(f32)
            rate = by_token(norms[it, owner])
            pairs.append((mixed * wide_scale(rate, 2 * kv_cols)).astype(bf16))
        pair = jnp.concatenate(pairs, axis=0)
        for e in range(kv_local):
            keys = pair[:, e * HEAD_DIM : (e + 1) * HEAD_DIM]
            values = pair[:, kv_cols + e * HEAD_DIM : kv_cols + (e + 1) * HEAD_DIM]
            values = jnp.concatenate([values, jnp.ones((2 * toks, HEAD_DIM), bf16)], axis=1)
            asked = queries[e * group : (e + 1) * group].reshape(group * toks, HEAD_DIM)
            scores = lax.dot_general(asked, keys, (((1,), (1,)), ((), ())), preferred_element_type=f32)
            scores = (scores.reshape(group, toks, 2 * toks) + bias[which][None]).reshape(group * toks, 2 * toks)
            old = top[e]
            new = jnp.maximum(old, jnp.max(scores, axis=1, keepdims=True))
            top[e] = new
            both = jnp.concatenate([new] * (2 * toks // lanes), axis=1)
            weights = jnp.exp2((scores - both) * factor)
            fade = jnp.exp2((old - new) * factor)
            acc[e] = acc[e] * jnp.concatenate([fade, fade], axis=1) + jnp.dot(
                weights.astype(bf16), values, preferred_element_type=f32
            )

    def near_step(c, d):
        return remote(
            near_out.at[d, :, columns(c, span)], near.at[d, :, columns(c, span)],
            near_s.at[c, d], near_r.at[c, d], "feat", partner,
        )

    def far_step(c, d):
        return remote(
            outgoing.at[d, :, columns(c, span)], far.at[d, :, columns(c, span)],
            far_s.at[c, d], far_r.at[c, d], "feat", 2 * lined[d] + side,
        )

    def out_dot(target, c):
        cols = pl.ds(pl.multiple_of(target * part + c * span, span), span)
        return jnp.dot(attended[...], w_o[:, cols], preferred_element_type=f32)

    def pass_on(c):
        cols = columns(c, span)
        for d in range(1, lines):
            near_step(c, d).wait_recv()
            outgoing[d, :, cols] = (keep[d, :, cols] + near[d, :, cols].astype(f32)).astype(bf16)
            far_step(c, d).start()

    def own_dots(c):
        cols = columns(c, span)
        near_out[0, :, cols] = out_dot(2 * mine + 1 - side, c).astype(bf16)
        near_step(c, 0).start()
        keep[0, :, cols] = out_dot(me, c)

    def arrive(it, c, k):
        @pl.when(k <= level)
        def _():
            owner = at_seq - 2 * k
            up_step(it, c, k - 1, owner, owner).wait_recv()

            @pl.when(level + 1 < levels)
            def _():
                up_step(it, c, k, owner, at_seq + 2).start()

            side_step(it, c, k, owner).start()

    def all_rows():
        return pl.ds(0, toks)

    def collect(p):
        gather_step(p, 0).wait()
        for d in range(1, lines):
            forward_step(p, d).wait()
            gather_step(p, d).wait_send()

    def send_keys(it, c):
        rows = pl.ds(c * half, half) if isinstance(c, int) else pl.ds(pl.multiple_of(c * half, half), half)
        for at in range(2 * kv_cols // kv_tile):
            cols = pl.ds(at * kv_tile, kv_tile)
            there = project(tok, rows, w_kv, cols) * wide_scale(scale_out[rows, :], kv_tile)
            kv[it, at_seq, rows, cols] = (there + base_proj[rows, cols]).astype(bf16)

        @pl.when(row_side == 0)
        def _():
            side_step(it, c, 0, at_seq).start()

        @pl.when(level + 1 < levels)
        def _():
            up_step(it, c, 0, at_seq, at_seq + 2).start()

    def ask(it, at):
        cols = columns(at, q_tile)
        there = project(tok, all_rows(), w_q, cols) * wide_scale(scale_out[...], q_tile)
        proj[it, :, cols] = there + base_proj[:, pl.ds(pl.multiple_of(2 * kv_cols + at * q_tile, q_tile), q_tile)]
        total = shares[0][:1, :1] * proj[0, :, cols]
        for j in range(1, ITERS):
            total = total + shares[j][:1, :1] * proj[j, :, cols]
        asked = (total * wide_scale(scale_in[...], q_tile)).astype(bf16)
        for h in range(q_tile // HEAD_DIM):
            queries[at * (q_tile // HEAD_DIM) + h] = asked[:, h * HEAD_DIM : (h + 1) * HEAD_DIM]

    def project_base():
        for d in range(1, lines):
            inj_forward(d).wait()
        inj_step(0).wait()
        for d in range(1, lines):
            inj_step(d).wait_send()

        @pl.loop(0, 2 * kv_cols // kv_tile)
        def _(at):
            cols = columns(at, kv_tile)
            base_proj[:, cols] = project(tok_inj, all_rows(), w_kv, cols)

        @pl.loop(0, head_cols // q_tile)
        def _(at):
            put = pl.ds(pl.multiple_of(2 * kv_cols + at * q_tile, q_tile), q_tile)
            base_proj[:, put] = project(tok_inj, all_rows(), w_q, columns(at, q_tile))

    hops = sorted(((c, k) for c in range(HALVES) for k in range(1, levels)), key=lambda one: one[0] + 3 * one[1])

    def evaluate(it):
        k = jnp.maximum(it - 1, 0)
        slot = lax.rem(it, 2)
        waiting = list(hops)
        met = []

        def forward(count):
            for c, j in waiting[:count]:
                arrive(it, c, j)
                waiting.remove((c, j))
                if all(other[1] != j for other in waiting):
                    met.append(j - 1)

        relay(0)
        relay(1)

        @pl.when(it > 0)
        def _():
            settle_first(k, slot)

        @pl.when(it == 0)
        def _():
            loads[2].wait()
            loads[3].wait()

        collect(0)
        collect(1)
        send_keys(it, 0)
        relay(2)

        @pl.loop(1, HALVES)
        def _(c):
            collect(c + 1)

            @pl.when(c + 1 < HALVES)
            def _():
                relay(c + 2)

            send_keys(it, c)

            @pl.when(c == HALVES - 2)
            def _():
                for one in waiting[:1]:
                    arrive(it, *one)

        del waiting[:1]
        forward(2)

        @pl.when(it > 0)
        def _():
            share_norms(it, settle_last(k, slot)[:1])
            shares[0] = jnp.zeros((8, lanes), f32)
            for j in range(1, ITERS):
                shares[j] = coef[j - 1]

        @pl.when(it == 0)
        def _():
            total = mail_total(1)
            dots[(INJ + 1) * WARM + WARM] = everywhere(total[:1])
            dots[(INJ + 1) * INJ + INJ] = everywhere(total[1:2])
            share_norms(it, inverse_rms(total[2:3]))
            loads[4].wait()
            for d in range(lines):
                inj_step(d).start()

        q_tiles = head_cols // q_tile
        early_hops = waiting[:q_tiles]

        @pl.loop(0, q_tiles)
        def _(at):
            ask(it, at)
            for index, one in enumerate(early_hops):
                @pl.when(at == index)
                def _():
                    arrive(it, *one)

        met.extend(sorted({j - 1 for c, j in early_hops if all(other[1] != j for other in waiting[q_tiles:])}))
        del waiting[:q_tiles]

        @pl.when(it > 0)
        def _():
            remix(k)

        for e in range(kv_local):
            top[e] = jnp.full(top.shape[1:], -1e30, f32)
            acc[e] = jnp.zeros(acc.shape[1:], f32)

        def meet(k):
            @pl.when(k <= level)
            def _():
                @pl.when(k + row_side > 0)
                def _():
                    for c in range(HALVES):
                        side_step(it, c, k, row_partner - 2 * k).wait_recv()

                for o in range(2):
                    d = 2 * k - o + row_side

                    @pl.when((d > 0) & (at_seq - d >= 0))
                    def _():
                        norm_step(it, d, at_seq, at_seq - d).wait_recv()

                attend(it, k)

        while waiting:
            for k in met:
                meet(k)
            met.clear()
            forward(1)
        for k in met + [levels - 1]:
            meet(k)

        for e in range(kv_local):
            for g in range(group):
                rows = slice(g * toks, (g + 1) * toks)
                at = (e * group + g) * HEAD_DIM
                attended[:, at : at + HEAD_DIM] = (
                    acc[e, rows, :HEAD_DIM] / acc[e, rows, HEAD_DIM:]
                ).astype(bf16)

        @pl.when(it == 0)
        def _():
            loads[5].wait()
            for d in range(1, lines):
                inj_step(d).wait_recv()
                inj_forward(d).start()

        @pl.loop(0, CHUNKS)
        def _(c):
            cols = columns(c, span)
            for d in range(1, lines):
                near_out[d, :, cols] = out_dot(2 * lined[d] + 1 - side, c).astype(bf16)
                near_step(c, d).start()
                keep[d, :, cols] = out_dot(2 * lined[d] + side, c)

            @pl.when(c > 0)
            def _():
                pass_on(c - 1)

        own_dots(0)
        pass_on(CHUNKS - 1)

        @pl.loop(1, CHUNKS)
        def _(c):
            own_dots(c)

        @pl.when(it == 0)
        def _():
            project_base()

        for at in range(ROWS):
            sums[at] = zero_tile

        @pl.loop(0, CHUNKS)
        def _(c):
            near_step(c, 0).wait()
            for d in range(1, lines):
                near_step(c, d).wait_send()
                far_step(c, d).wait()
            for at in range(span // lanes):
                cols = pl.ds(pl.multiple_of(c * span + at * lanes, lanes), lanes)
                update = keep[0, :, cols] + near[0, :, cols].astype(f32)
                for d in range(1, lines):
                    update = update + far[d, :, cols].astype(f32)
                base = inj[:, cols].astype(f32)
                summed = out[:, cols] + base + update
                held[:, cols] = summed
                scaled = summed * gain_out[me, :, cols]
                tok[me, :, cols] = (scaled * gain_in[me, :, cols]).astype(bf16)
                others = [images[j, :, cols] for j in range(ITERS - 1)]
                others = others + [warm[:, cols].astype(f32), base, scaled]
                sums[0] += summed * summed
                for row, other in enumerate(others):
                    sums[row + 1] += scaled * other

            @pl.when((it + 1 < ITERS) & (c == CHUNKS - 2))
            def _():
                start_gather(0)

        mail_out[0] = row_sums([sums[at] for at in range(ROWS)])
        mail_start(0)

        @pl.when(it + 1 < ITERS)
        def _():
            for p in range(1, count):
                start_gather(p)

        for c in range(HALVES):
            @pl.when(row_side == 0)
            def _():
                side_step(it, c, 0, at_seq).wait_send()

            @pl.when(level + 1 < levels)
            def _():
                up_step(it, c, 0, at_seq, at_seq + 2).wait_send()

        @pl.loop(1, level + 1)
        def _(k):
            for c in range(HALVES):
                side_step(it, c, k, at_seq - 2 * k).wait_send()

                @pl.when(level + 1 < levels)
                def _():
                    up_step(it, c, k, at_seq - 2 * k, at_seq + 2).wait_send()

        for d in range(1, m):
            @pl.when(at_seq + d < m)
            def _():
                norm_step(it, d, at_seq, at_seq + d).wait_send()

    @pl.loop(0, ITERS)
    def _(it):
        evaluate(it)

    settle_first(ITERS - 1, lax.rem(ITERS, 2))
    settle_last(ITERS - 1, lax.rem(ITERS, 2))
    remix(ITERS - 1)


def on_device(injection, warm_start, gain_in, gain_out, w_query, w_key, w_value, w_out):
    n, m = lax.axis_size("feat"), lax.axis_size("seq")
    toks, part = injection.shape
    head_cols, kv_cols = w_query.shape[1], w_key.shape[1]
    kv_local = kv_cols // HEAD_DIM
    group = HEADS // KV_HEADS
    lines = n // 2
    f32, bf16 = jnp.float32, jnp.bfloat16
    vmem, dma = pltpu.VMEM, pltpu.SemaphoreType.DMA
    lanes = 128
    scratch = [
        vmem((n, toks, part), bf16), vmem((n, toks, part), bf16),
        vmem((w_key.shape[0], 2 * kv_cols), bf16), vmem(w_query.shape, bf16), vmem(w_out.shape, bf16),
        vmem((toks, part), bf16), vmem((toks, part), bf16),
        vmem((ITERS, toks, part), f32), vmem((toks, part), f32),
        vmem((ITERS, toks, head_cols), f32), vmem((toks, head_cols + 2 * kv_cols), f32),
        vmem((head_cols // HEAD_DIM, toks, HEAD_DIM), bf16),
        vmem((ITERS, m, toks, 2 * kv_cols), bf16),
        vmem((kv_local, group * toks, 2 * HEAD_DIM), f32), vmem((kv_local, group * toks, lanes), f32),
        vmem((2, toks, 2 * toks), f32), vmem((toks, head_cols), bf16),
        vmem((lines, toks, part), f32),
        vmem((lines, toks, part), bf16), vmem((lines, toks, part), bf16),
        vmem((lines, toks, part), bf16), vmem((lines, toks, part), bf16),
        vmem((ITERS, 8, lanes), f32), vmem((ITERS, 8, lanes), f32), vmem((ITERS * ITERS, 8, lanes), f32),
        vmem(((INJ + 1) * (INJ + 1), 8, toks), f32), vmem(((WARM + 1) * (WARM + 1), 8, lanes), f32),
        vmem((ITERS * (WARM + 1), 8, lanes), f32), vmem((ROWS, toks, lanes), f32),
        vmem((8, toks), f32), vmem((ITERS, m, 8, toks), f32),
        vmem((toks, lanes), f32), vmem((toks, lanes), f32),
        vmem((3, 8, toks), f32), vmem((3, n, 8, toks), f32),
        vmem((8, lanes), f32), vmem((2, m, 8, lanes), f32),
        dma((6,)), dma((HALVES + 1, n)), dma((HALVES + 1, n)), dma((n,)), dma((n,)),
        dma((HALVES, m // 2)), dma((ITERS, HALVES, m // 2)), dma((HALVES, m // 2)), dma((ITERS, HALVES, m // 2)),
        dma((CHUNKS, lines)), dma((CHUNKS, lines)), dma((CHUNKS, lines)), dma((CHUNKS, lines)),
        dma((3, n)), dma((3, n)), dma((2, m)), dma((2, m)), dma((m,)), dma((ITERS, m)),
    ]
    return pl.pallas_call(
        functools.partial(whole_kernel, n, m),
        out_shape=jax.ShapeDtypeStruct((toks, part), f32),
        in_specs=[ANY, ANY, VMEM, VMEM, ANY, ANY, ANY, ANY],
        out_specs=VMEM,
        scratch_shapes=scratch,
        compiler_params=pltpu.CompilerParams(
            collective_id=0, has_side_effects=True, vmem_limit_bytes=63 * 1024 * 1024
        ),
    )(
        injection, warm_start, gain_in.reshape(n, 1, part), gain_out.reshape(n, 1, part),
        w_query, w_key, w_value, w_out,
    )


def solution(mesh):
    in_specs = (
        P("seq", "feat"),
        P("seq", "feat"),
        P(),
        P(),
        P(None, "feat"),
        P(None, "feat"),
        P(None, "feat"),
        P("feat", None),
    )
    out_specs = P("seq", "feat")
    return jax.shard_map(
        on_device, mesh=mesh, in_specs=in_specs, out_specs=out_specs, check_vma=False
    )
```
